128 devices in a mesh: gx: 16 (over x, z), gy: 8 (over y, core).
Axes of the slice: x: 4, y: 4, z: 4, core: 2. Of those that a mesh axis runs over, the one named last changes fastest.
Arguments:
- tokens: bfloat16 [512, 8192], P(None, 'gx'), may hold values from -16 to 16
- attn_gain: bfloat16 [8192], P('gx'), may hold values from 0.25 to 1.75
- qkv_weight: bfloat16 [8192, 10240], P('gx', 'gy'), may hold values from -0.0625 to 0.0625
- cache_keys: bfloat16 [512, 8, 512, 128], P('gx', 'gy'), may hold values from -160 to 160
- cache_values: bfloat16 [512, 8, 512, 128], P('gx', 'gy'), may hold values from -6 to 6
- lengths: int32 [512], replicated, may hold values from 1 to 512
- live_mask: int32 [512], replicated, may hold values 0 or 1
- out_weight: bfloat16 [8192, 8192], P('gy', 'gx'), may hold values from -0.0625 to 0.0625
- mlp_gain: bfloat16 [8192], P('gx'), may hold values from 0.25 to 1.75
- gate_weight: bfloat16 [8192, 28672], P('gx', 'gy'), may hold values from -0.0625 to 0.0625
- up_weight: bfloat16 [8192, 28672], P('gx', 'gy'), may hold values from -0.0625 to 0.0625
- down_weight: bfloat16 [28672, 8192], P('gy', 'gx'), may hold values from -0.03125 to 0.03125
Outputs:
- updated: bfloat16 [512, 8192], P('gy', 'gx')
The draws below stay inside these ranges and needn't reach their ends.
All inputs are finite; a program needn't handle non-finite values.
Results may differ from the reference program's by a relative error of at most 0.0095.
Values may be sent and summed in bfloat16 or wider, within the bound.
A program may use at most 128 MiB of HBM per device.

```python
import jax
import jax.numpy as jnp
from jax import lax

D = 8192
H = 64
KVH = 8
HD = 128
FF = 28672
CACHE = 512
BATCH = 512


def draw_tokens(key, part):
    key_cols, key_base, key_rows, key_common = jax.random.split(jax.random.fold_in(key, 11), 4)
    block_width = D // 32
    col_scale = jnp.exp(jax.random.uniform(key_cols, (32,), jnp.float32, -0.9, 0.9))
    col_scale = jnp.repeat(col_scale, block_width)[None, :]
    base_draw = jax.random.normal(key_base, (BATCH, D), jnp.float32)
    values = base_draw * col_scale
    return jnp.clip(values, -16.0, 16.0).astype(jnp.bfloat16)


def draw_cache_keys(key, part):
    key_base, key_pick, key_sign = jax.random.split(jax.random.fold_in(key, 23), 3)
    dims_all = (BATCH, KVH, CACHE, HD)
    values = jnp.clip(jax.random.normal(key_base, dims_all, jnp.float32), -6.0, 6.0)
    return values.astype(jnp.bfloat16)


def plant(array, key, low, largest):
    index_at = [jax.random.randint(jax.random.fold_in(key, axis), (), 0, length) for axis, length in enumerate(array.shape)]
    longest = array.shape.index(max(array.shape))
    beside = index_at[:longest] + [(index_at[longest] + 1) % array.shape[longest]] + index_at[longest + 1:]
    return array.at[tuple(index_at)].set(low).at[tuple(beside)].set(largest)


def block_scale(key, shape, shards, least, largest):
    level = 1.0
    for axis_at, parts in shards:
        draws = jax.random.uniform(jax.random.fold_in(jax.random.fold_in(key, 6), axis_at), (parts,), jnp.float32, least / len(shards), largest / len(shards))
        level = level * jnp.repeat(jnp.exp(draws), shape[axis_at] // parts).reshape((-1,) + (1,) * (len(shape) - 1 - axis_at))
    return level


def noise(stream_key, dims, width, bound, shards=(), held_as=jnp.bfloat16):
    values = jax.random.normal(stream_key, dims, jnp.float32) * width
    if len(shards) > 0:
        values = block_scale(stream_key, dims, shards, -0.22, 0.18) * values
    return jnp.clip(values, min=-bound, max=bound).astype(held_as)


def setup_inputs(seed: int = 0) -> dict:
    splits = jax.random.split(jax.random.key(seed), 13)
    tokens = draw_tokens(jax.random.fold_in(splits[12], 71), 0)
    attn_gain = jnp.clip(1.0 + 0.15 * jax.random.normal(splits[1], (D,), jnp.float32), 0.25, 1.75).astype(jnp.bfloat16)
    qkv_weight = noise(splits[2], (D, KVH * (H // KVH + 2) * HD), D ** -0.5, 0.0625, ((0, 16), (1, 8)))
    cache_keys = draw_cache_keys(jax.random.fold_in(splits[12], 71), 0)
    cache_values = noise(splits[4], (BATCH, KVH, CACHE, HD), 1.0, 6.0, ((0, 16), (1, 8)))
    lengths = plant(jax.random.randint(splits[5], (BATCH,), 1, CACHE + 1), jax.random.fold_in(splits[5], 1), 1, CACHE).astype(jnp.int32)
    live_mask = plant((jax.random.randint(splits[6], (BATCH,), 0, 4) < 3).astype(jnp.int32), jax.random.fold_in(splits[6], 1), 0, 1)
    out_weight = noise(splits[7], (H * HD, D), (H * HD) ** -0.5, 0.0625, ((0, 8), (1, 16)))
    mlp_gain = jnp.clip(1.0 + 0.15 * jax.random.normal(splits[8], (D,), jnp.float32), 0.25, 1.75).astype(jnp.bfloat16)
    gate_weight = noise(splits[9], (D, FF), D ** -0.5, 0.0625, ((0, 16), (1, 8)))
    up_weight = noise(splits[10], (D, FF), D ** -0.5, 0.0625, ((0, 16), (1, 8)))
    down_weight = noise(splits[11], (FF, D), FF ** -0.5, 0.03125, ((0, 8), (1, 16)))
    return {"tokens": tokens, "attn_gain": attn_gain, "qkv_weight": qkv_weight, "cache_keys": cache_keys, "cache_values": cache_values, "lengths": lengths, "live_mask": live_mask, "out_weight": out_weight, "mlp_gain": mlp_gain, "gate_weight": gate_weight, "up_weight": up_weight, "down_weight": down_weight}


ROPE_BASE = 500000.0
NORM_EPS = 1e-05
MASKED = -1e+30

def rotate_pairs(vectors, positions):
    half_width = vectors.shape[-1] // 2
    index_float = jnp.arange(half_width).astype(jnp.float32)
    inv_freq = jnp.exp(index_float * (-2.0 * jnp.log(ROPE_BASE) / vectors.shape[-1]))
    angles = positions.astype(jnp.float32)[:, None] * inv_freq[None, :]
    cosine = jnp.cos(angles)[:, None, :]
    sine_part = jnp.sin(angles)[:, None, :]
    low_half = vectors[..., :half_width]
    high_half = vectors[..., half_width:]
    return jnp.concatenate((low_half * cosine - high_half * sine_part, high_half * cosine + low_half * sine_part), axis=-1)

def attend_group(query_rows, fresh_key_rows, new_values, grouped_key_rows, grouped_value_rows, lengths):
    score_scale = query_rows.shape[-1] ** (-0.5)
    stored_entries = jnp.einsum('whj,wpj->whp', query_rows.astype(jnp.float32), grouped_key_rows.astype(jnp.float32)) * score_scale
    valid = jnp.arange(grouped_key_rows.shape[1])[None, None, :] < lengths[:, None, None]
    stored_entries = jnp.where(valid, stored_entries, MASKED)
    self_token = jnp.einsum('rnj,rj->rn', query_rows.astype(jnp.float32), fresh_key_rows.astype(jnp.float32)) * score_scale
    peak = jnp.maximum(lax.optimization_barrier(jnp.max(stored_entries, axis=-1)), self_token)
    attention_probs = jnp.where(valid, jnp.exp(stored_entries - peak[..., None]), 0.0).astype(jnp.bfloat16)
    own_weight = jnp.exp(self_token - peak).astype(jnp.bfloat16)
    totals = lax.optimization_barrier(jnp.sum(attention_probs.astype(jnp.float32), axis=-1)) + own_weight.astype(jnp.float32)
    blended_values = jnp.einsum('zcx,zxr->zcr', attention_probs.astype(jnp.float32), grouped_value_rows.astype(jnp.float32))
    blended_values = blended_values + own_weight.astype(jnp.float32)[..., None] * new_values.astype(jnp.float32)[:, None, :]
    return (blended_values / totals[..., None]).astype(jnp.bfloat16)

def reference(tokens, attn_gain, qkv_weight, cache_keys, cache_values, lengths, live_mask, out_weight, mlp_gain, gate_weight, up_weight, down_weight):
    rows_all = tokens.shape[0]
    per_kv = H // KVH
    wide_in = tokens.astype(jnp.float32)
    attn_scale = lax.rsqrt(lax.optimization_barrier(jnp.sum(wide_in * wide_in, axis=1)) / D + NORM_EPS)
    scaled = (wide_in * attn_gain.astype(jnp.float32)).astype(jnp.bfloat16)
    projected = jnp.dot(scaled, qkv_weight, preferred_element_type=jnp.float32) * attn_scale[:, None]
    projected = projected.reshape(rows_all, KVH, per_kv + 2, HD)
    query_rows = rotate_pairs(projected[:, :, :per_kv].reshape(rows_all, H, HD), lengths)
    query_rows = query_rows.astype(jnp.bfloat16).reshape(rows_all, KVH, per_kv, HD)
    fresh_key_rows = rotate_pairs(projected[:, :, per_kv], lengths).astype(jnp.bfloat16)
    new_values = projected[:, :, per_kv + 1].astype(jnp.bfloat16)

    def one_group(group_index):
        query_group = lax.dynamic_index_in_dim(query_rows, group_index, 1, keepdims=False)
        key_new = lax.dynamic_index_in_dim(fresh_key_rows, group_index, 1, keepdims=False)
        value_new = lax.dynamic_index_in_dim(new_values, group_index, 1, keepdims=False)
        grouped_key_rows = lax.dynamic_index_in_dim(cache_keys, group_index, 1, keepdims=False)
        grouped_value_rows = lax.dynamic_index_in_dim(cache_values, group_index, 1, keepdims=False)
        return attend_group(query_group, key_new, value_new, grouped_key_rows, grouped_value_rows, lengths)
    grouped = lax.map(one_group, jnp.arange(KVH).astype(jnp.int32))
    attn = jnp.transpose(grouped, (1, 0, 2, 3)).reshape(rows_all, H * HD)
    attn_proj = jnp.dot(attn, out_weight, preferred_element_type=jnp.float32)
    alive_col = live_mask.astype(jnp.float32)[:, None]
    residual = (wide_in + alive_col * attn_proj).astype(jnp.bfloat16)
    resid_wide = residual.astype(jnp.float32)
    mlp_scale = lax.rsqrt(lax.optimization_barrier(jnp.sum(resid_wide * resid_wide, axis=1)) / D + NORM_EPS)
    mlp_in = (resid_wide * mlp_gain.astype(jnp.float32)).astype(jnp.bfloat16)
    gate_sum = jnp.dot(mlp_in, gate_weight, preferred_element_type=jnp.float32) * mlp_scale[:, None]
    up_sum = jnp.dot(mlp_in, up_weight, preferred_element_type=jnp.float32) * mlp_scale[:, None]
    hidden = (jax.nn.silu(gate_sum) * up_sum).astype(jnp.bfloat16)
    down_sum = jnp.dot(hidden, down_weight, preferred_element_type=jnp.float32)
    return (resid_wide + alive_col * down_sum).astype(jnp.bfloat16)
```

```python
import math

import jax
import jax.numpy as jnp
from jax import lax
from jax.experimental import pallas as pl
from jax.experimental.pallas import tpu as pltpu
from jax.sharding import Mesh
from jax.sharding import PartitionSpec as P

D = 8192
HD = 128
GX = ("x", "z")
GY = ("y", "c")
MESH = pl.DeviceIdType.MESH
F32 = jnp.float32
BF16 = jnp.bfloat16

ROPE_BASE = 500000.0
NORM_EPS = 1e-05
MASKED = -1e30

MLP_CHUNKS = 7
STRAIGHT = (0, 0, 0, 0)


def send(src, dst, send_sem, recv_sem, device):
    pltpu.make_async_remote_copy(
        src_ref=src,
        dst_ref=dst,
        send_sem=send_sem,
        recv_sem=recv_sem,
        device_id=device,
        device_id_type=MESH,
    ).start()


def wait_bytes(ref, sem):
    pltpu.make_async_copy(ref, ref, sem).wait()


class Ring:
    def __init__(self, axis):
        self.me = lax.axis_index(axis)
        self.places = [lax.rem(self.me + r, 4) for r in range(4)]
        self.right, self.far, self.left = self.places[1:]
        self.devices = [{axis: place} for place in self.places]
        self.to_right, self.to_far, self.to_left = self.devices[1:]


def scatter_direct(ring, block, into, ssem, rsem):
    for r in (2, 1, 3):
        send(block(ring.places[r]), into(r - 1), ssem, rsem, ring.devices[r])


def gather_direct(ring, whole, ssem, rsem):
    for r in (2, 1, 3):
        send(whole(ring.me), whole(ring.me), ssem, rsem(r - 1), ring.devices[r])


def scatter_start(ring, block, from_far, from_near, ssem, rsem, direct=False):
    if direct:
        for half in range(2):
            send(block(ring.far, half), from_far(half), ssem, rsem(half), ring.to_far)
        for half in range(2):
            send(block(ring.right, half), from_near(0, half), ssem, rsem(2), ring.to_right)
            send(block(ring.left, half), from_near(1, half), ssem, rsem(3), ring.to_left)
        return
    send(block(ring.far, 0), from_far(0), ssem, rsem(0), ring.to_right)
    send(block(ring.far, 1), from_far(1), ssem, rsem(1), ring.to_left)
    send(block(ring.right, 1), from_near(0, 1), ssem, rsem(2), ring.to_right)
    send(block(ring.left, 0), from_near(1, 0), ssem, rsem(3), ring.to_left)


def scatter_forward(ring, block, from_far, from_near, ssem, rsem):
    for way, place, device in ((0, ring.right, ring.to_right), (1, ring.left, ring.to_left)):
        wait_bytes(from_far(way), rsem(way))
        mine = block(place, way)
        mine[...] = (mine[...].astype(F32) + from_far(way)[...].astype(F32)).astype(BF16)
        send(mine, from_near(way, way), ssem, rsem(2 + way), device)


def scatter_finish(own, near, far, rsem):
    total = own.astype(F32)
    if far is not None:
        for way in range(2):
            wait_bytes(far(way), rsem(way))
        total = total + jnp.concatenate([far(0)[...].astype(F32), far(1)[...].astype(F32)], axis=0)
    for way in range(2):
        wait_bytes(near(way), rsem(2 + way))
    return total + near(0)[...].astype(F32) + near(1)[...].astype(F32)


def gather_start(ring, whole, block, ssem, rsem, direct=False):
    if direct:
        for half in range(2):
            send(block(ring.me, half), block(ring.me, half), ssem, rsem(2 + half), ring.to_far)
    send(whole(ring.me), whole(ring.me), ssem, rsem(0), ring.to_right)
    send(whole(ring.me), whole(ring.me), ssem, rsem(1), ring.to_left)


def gather_forward(ring, whole, block, ssem, rsem):
    wait_bytes(whole(ring.left), rsem(0))
    send(block(ring.left, 0), block(ring.left, 0), ssem, rsem(2), ring.to_right)
    wait_bytes(whole(ring.right), rsem(1))
    send(block(ring.right, 1), block(ring.right, 1), ssem, rsem(3), ring.to_left)


def gather_finish(ring, whole, block, rsem, direct=False):
    if direct:
        wait_bytes(whole(ring.left), rsem(0))
        wait_bytes(whole(ring.right), rsem(1))
    wait_bytes(block(ring.far, 0), rsem(2))
    wait_bytes(block(ring.far, 1), rsem(3))


def greet(devices):
    barrier = pltpu.get_barrier_semaphore()
    for device in devices:
        pl.semaphore_signal(barrier, inc=1, device_id=device, device_id_type=MESH)
    return lambda: pl.semaphore_wait(barrier, len(devices))


def row_squares(wide):
    squares = wide * wide
    high = squares.astype(BF16)
    low = (squares - high.astype(F32)).astype(BF16)
    ones = jnp.ones((8, wide.shape[1]), BF16)
    dims = (((1,), (1,)), ((), ()))
    return lax.dot_general(ones, high, dims, preferred_element_type=F32) + lax.dot_general(
        ones, low, dims, preferred_element_type=F32
    )


def as_column(lanes, count, first):
    shape = (count, lanes.shape[1])
    lane = lax.broadcasted_iota(jnp.int32, shape, 1)
    row = lax.broadcasted_iota(jnp.int32, shape, 0)
    return jnp.sum(jnp.where(lane == row + first, lanes, 0.0), axis=1, keepdims=True)


class Squares:
    def __init__(self, rings, sq, sq_x, sq_mid, sq_z, sems):
        self.rings, self.refs, self.sems = rings, (sq, sq_x, sq_mid, sq_z), sems

    def over_x(self):
        sq, sq_x, _, _ = self.refs
        scatter_direct(
            self.rings[0], lambda d: sq.at[d], lambda i: sq_x.at[i], self.sems.at[0], self.sems.at[1]
        )

    def over_z(self):
        sq, sq_x, sq_mid, sq_z = self.refs
        wait_bytes(sq_x, self.sems.at[1])
        sq_mid[...] = sq[self.rings[0].me] + jnp.sum(sq_x[...], axis=0)
        scatter_direct(
            self.rings[1], lambda d: sq_mid, lambda i: sq_z.at[i], self.sems.at[2], self.sems.at[3]
        )

    def scale(self):
        _, _, sq_mid, sq_z = self.refs
        wait_bytes(sq_z, self.sems.at[3])
        total = sq_mid[...] + jnp.sum(sq_z[...], axis=0)
        sums = as_column(total[0:1, :], 32, 32 * self.rings[1].me)
        return lax.rsqrt(sums / D + NORM_EPS)

    def drain(self):
        wait_bytes(self.refs[1], self.sems.at[0])
        wait_bytes(self.refs[3], self.sems.at[2])


def either(k, chunks, straight, work):
    if straight == 0:
        work(False)
        return

    @pl.when(k < chunks - straight)
    def _():
        work(False)

    @pl.when(k >= chunks - straight)
    def _():
        work(True)


def run_stages(count, stages):
    def body(t, carry):
        for lag, stage in enumerate(stages):
            k = t - lag

            @pl.when((k >= 0) & (k < count))
            def _():
                stage(k)

        return carry

    lax.fori_loop(0, count + len(stages) - 1, body, 0)


def scatter_stages(rings, part, far1, near1, sum1, far2, near2, ssem, rsem):
    def block1(h, k):
        return lambda d, half: part.at[h, k, d, pl.ds(2 * half, 2)]

    def far_in1(h, k):
        return lambda way: far1.at[h, k, way]

    def near_in1(h, k):
        return lambda way, half: near1.at[h, k, way, pl.ds(2 * half, 2)]

    def block2(h, k):
        return lambda d, half: sum1.at[h, k, d, pl.ds(16 * half, 16)]

    def far_in2(h, k):
        return lambda way: far2.at[h, k, way]

    def near_in2(h, k):
        return lambda way, half: near2.at[h, k, way, pl.ds(16 * half, 16)]

    def rs(h, k, base):
        return lambda i: rsem.at[k, h, base + i]

    chunks = part.shape[1]

    def start1(k):
        def work(direct):
            for h in range(2):
                refs = (block1(h, k), far_in1(h, k), near_in1(h, k))
                scatter_start(rings[h], *refs, ssem.at[k, h, 0], rs(h, k, 0), direct)

        either(k, chunks, STRAIGHT[0], work)

    def forward1(k):
        @pl.when(k < chunks - STRAIGHT[0])
        def _():
            for h in range(2):
                refs = (block1(h, k), far_in1(h, k), near_in1(h, k))
                scatter_forward(rings[h], *refs, ssem.at[k, h, 0], rs(h, k, 0))

    def start2(k):
        def total(direct):
            for h in range(2):
                own = part[h, k, rings[h].me]
                far = far_in1(h, k) if direct else None
                got = scatter_finish(own, lambda way: near1.at[h, k, way], far, rs(h, k, 0))
                sum1[h, k] = got.astype(BF16)

        def work(direct):
            for h in range(2):
                refs = (block2(h, k), far_in2(h, k), near_in2(h, k))
                scatter_start(rings[1 - h], *refs, ssem.at[k, h, 1], rs(h, k, 4), direct)

        either(k, chunks, STRAIGHT[0], total)
        either(k, chunks, STRAIGHT[1], work)

    def forward2(k):
        @pl.when(k < chunks - STRAIGHT[1])
        def _():
            for h in range(2):
                refs = (block2(h, k), far_in2(h, k), near_in2(h, k))
                scatter_forward(rings[1 - h], *refs, ssem.at[k, h, 1], rs(h, k, 4))

    def finish2(h, k, direct):
        own = sum1[h, k, rings[1 - h].me]
        far = far_in2(h, k) if direct else None
        return scatter_finish(own, lambda way: near2.at[h, k, way], far, rs(h, k, 4))

    return start1, forward1, start2, forward2, finish2


def scatter_scratch(chunks, width):
    return [
        pltpu.VMEM((2, chunks, 4, 4, 32, width), BF16),
        pltpu.VMEM((2, chunks, 2, 2, 32, width), BF16),
        pltpu.VMEM((2, chunks, 2, 4, 32, width), BF16),
        pltpu.VMEM((2, chunks, 4, 32, width), BF16),
        pltpu.VMEM((2, chunks, 2, 16, width), BF16),
        pltpu.VMEM((2, chunks, 2, 32, width), BF16),
    ]


def gather_stages(rings, buf, ssem, rsem):
    def inner(h, k):
        ring = rings[1 - h]
        row = rings[h].me
        return (
            ring,
            lambda d: buf(h, k).at[row, d],
            lambda d, half: buf(h, k).at[row, d, pl.ds(16 * half, 16)],
        )

    def outer(h, k):
        return (
            rings[h],
            lambda d: buf(h, k).at[d],
            lambda d, half: buf(h, k).at[d, pl.ds(2 * half, 2)],
        )

    chunks = MLP_CHUNKS

    def start1(h, k, direct):
        ring, whole, block = inner(h, k)
        gather_start(ring, whole, block, ssem(h, k, 0), lambda i: rsem(h, k, i), direct)

    def forward1(k):
        @pl.when(k < chunks - STRAIGHT[2])
        def _():
            for h in range(2):
                ring, whole, block = inner(h, k)
                gather_forward(ring, whole, block, ssem(h, k, 0), lambda i: rsem(h, k, i))

    def start2(k):
        def finish(direct):
            for h in range(2):
                ring, whole, block = inner(h, k)
                gather_finish(ring, whole, block, lambda i: rsem(h, k, i), direct)

        def work(direct):
            for h in range(2):
                ring, whole, block = outer(h, k)
                gather_start(ring, whole, block, ssem(h, k, 1), lambda i: rsem(h, k, 4 + i), direct)

        either(k, chunks, STRAIGHT[2], finish)
        either(k, chunks, STRAIGHT[3], work)

    def forward2(k):
        @pl.when(k < chunks - STRAIGHT[3])
        def _():
            for h in range(2):
                ring, whole, block = outer(h, k)
                gather_forward(ring, whole, block, ssem(h, k, 1), lambda i: rsem(h, k, 4 + i))

    def finish2(k):
        def finish(direct):
            for h in range(2):
                ring, whole, block = outer(h, k)
                gather_finish(ring, whole, block, lambda i: rsem(h, k, 4 + i), direct)

        either(k, chunks, STRAIGHT[3], finish)

    def drain(h, k):
        wait_bytes(buf(h, k).at[0, pl.ds(0, 3)], ssem(h, k, 0))
        wait_bytes(buf(h, k).at[pl.ds(0, 3)], ssem(h, k, 1))

    return start1, forward1, start2, forward2, finish2, drain


def columns_sum(acc, full, mine, core_in, ring, y_in, ssem, rsem):
    core = lax.axis_index("c")
    for b in range(16):
        a, c = divmod(b, 4)
        both = acc[0, a, c] + acc[1, c, a]
        full[(b // 2) % 2, b // 4, pl.ds(32 * (b % 2), 32)] = both.astype(BF16)
    for r in (2, 1, 3, 0):
        place = ring.places[r]
        send(full.at[1 - core, place], core_in.at[place], ssem.at[0], rsem.at[r], {"c": 1 - core})
    for r in (2, 1, 3, 0):
        place = ring.places[r]
        wait_bytes(core_in.at[place], rsem.at[r])
        both = full[core, place].astype(F32) + core_in[place].astype(F32)
        if r == 0:
            total = both
        else:
            mine[place] = both.astype(BF16)
            send(mine.at[place], y_in.at[r - 1], ssem.at[1], rsem.at[4], ring.devices[r])
    wait_bytes(y_in, rsem.at[4])
    total = total + jnp.sum(y_in[...].astype(F32), axis=0)
    wait_bytes(core_in, ssem.at[0])
    wait_bytes(y_in, ssem.at[1])
    return total


def gather_plane(rings, buf, ssem, rsem):
    def block(h, r):
        return buf.at[h, rings[h].me, rings[1 - h].places[r]]

    def outward(h, r):
        for way in (2, 1, 3):
            send(block(h, r), block(h, r), ssem.at[h], rsem.at[h, 2 + way], rings[h].devices[way])

    for h in range(2):
        for way in (2, 1, 3):
            device = rings[1 - h].devices[way]
            send(block(h, 0), block(h, 0), ssem.at[h], rsem.at[h, way - 1], device)
    for h in range(2):
        outward(h, 0)
    for way in (1, 3, 2):
        for h in range(2):
            wait_bytes(block(h, 4 - way), rsem.at[h, way - 1])
            outward(h, 4 - way)

    def finish(h):
        for way in (1, 3, 2):
            wait_bytes(buf.at[h, rings[h].places[4 - way]], rsem.at[h, 2 + way])

    def drain(h):
        wait_bytes(buf.at[h, 0, pl.ds(0, 3)], ssem.at[h])
        wait_bytes(buf.at[h, pl.ds(0, 3)], ssem.at[h])

    return finish, drain


def rotation(places):
    lane = lax.broadcasted_iota(jnp.int32, (1, HD), 1)
    index = lax.rem(lane, HD // 2).astype(F32)
    inv_freq = jnp.exp(index * (-2.0 * math.log(ROPE_BASE) / HD))
    angles = places * inv_freq
    sine = jnp.sin(angles)
    return jnp.cos(angles), jnp.where(lane < HD // 2, -sine, sine)


def layer_kernel(
    tok,
    attn_gain,
    mlp_gain,
    lengths,
    live_mask,
    w_qkv,
    keys,
    values,
    w_out,
    w_gate,
    w_up,
    w_down,
    base,
    extra,
    v_tok,
    v_qkv,
    v_keys,
    v_values,
    v_out,
    v_gate,
    v_up,
    v_down,
    q_part,
    q_in1,
    q_sum1,
    q_in2,
    sq0,
    sq0_x,
    sq0_mid,
    sq0_z,
    query,
    fresh,
    attended,
    lhs,
    abuf,
    acc,
    full,
    mine,
    core_in,
    y_in,
    full2,
    mine2,
    core_in2,
    y_in2,
    resid,
    part,
    far1,
    near1,
    sum1,
    far2,
    near2,
    hid,
    sq,
    sq_x,
    sq_mid,
    sq_z,
    scales,
    wsem,
    q_ssem,
    q_rsem,
    sqs0,
    a_ssem,
    a_rsem,
    y_ssem,
    y_rsem,
    r_ssem,
    r_rsem,
    sqs,
    m_ssem,
    m_rsem,
):
    rings = (Ring("x"), Ring("z"))
    yring = Ring("y")
    core = lax.axis_index("c")
    chunks, width = part.shape[1], part.shape[5]
    cut = width // 2
    depth = lhs.shape[4]
    slot0 = 32 * (4 * rings[0].me + rings[1].me)
    row0 = 64 * (2 * yring.me + core)
    loads = [
        pltpu.make_async_copy(src, dst, wsem.at[i])
        for i, (src, dst) in enumerate(
            (
                (tok, v_tok),
                (w_qkv, v_qkv),
                (keys, v_keys),
                (values, v_values),
                (w_out, v_out),
                (w_gate, v_gate),
                (w_up, v_up),
                (w_down, v_down),
            )
        )
    ]
    loads[0].start()
    loads[1].start()
    met = greet(
        [*rings[0].devices[1:], *rings[1].devices[1:], *yring.devices[1:], {"c": 1 - core}]
    )

    def row(ref):
        return ref[...].astype(F32).reshape(1, ref.shape[0])

    def normed(a, wide, gain, squares):
        squares[a] = row_squares(wide)
        scaled = (wide * gain).astype(BF16).reshape(4, 32, depth)
        lhs[0, a] = scaled
        for b in range(4):
            lhs[1, b, a] = scaled[b]

    loads[0].wait()
    for a in range(4):
        normed(a, v_tok[128 * a : 128 * (a + 1), :].astype(F32), row(attn_gain), sq0)
    loads[1].wait()
    for load in loads[2:]:
        load.start()
    q_width = q_part.shape[4]
    for h in range(2):
        columns = slice(h * q_width, (h + 1) * q_width)
        got = jnp.dot(lhs[h].reshape(512, depth), v_qkv[:, columns], preferred_element_type=F32)
        q_part[h] = got.astype(BF16).reshape(4, 4, 32, q_width)
    squares0 = Squares(rings, sq0, sq0_x, sq0_mid, sq0_z, sqs0)
    squares = Squares(rings, sq, sq_x, sq_mid, sq_z, sqs)
    met()
    for h in range(2):
        scatter_direct(
            rings[h],
            lambda d: q_part.at[h, d],
            lambda i: q_in1.at[h, i],
            q_ssem.at[h, 0],
            q_rsem.at[h, 0],
        )
    squares0.over_x()
    places = as_column(row(lengths), 32, slot0)
    cosine, sine = rotation(places)
    squares0.over_z()
    for h in range(2):
        wait_bytes(q_in1.at[h], q_rsem.at[h, 0])
        total = q_part[h, rings[h].me].astype(F32)
        for i in range(3):
            total = total + q_in1[h, i].astype(F32)
        q_sum1[h] = total.astype(BF16)
        scatter_direct(
            rings[1 - h],
            lambda d: q_sum1.at[h, d],
            lambda i: q_in2.at[h, i],
            q_ssem.at[h, 1],
            q_rsem.at[h, 1],
        )
    scale = squares0.scale()
    for h in range(2):
        wait_bytes(q_in2.at[h], q_rsem.at[h, 1])
        total = q_sum1[h, rings[1 - h].me].astype(F32)
        for i in range(3):
            total = total + q_in2[h, i].astype(F32)
        sums = total * scale
        for i in range(5):
            column = sums[:, 128 * i : 128 * (i + 1)]
            head = 5 * h + i
            if head < 9:
                column = column * cosine + pltpu.roll(column, HD // 2, 1) * sine
            column = column.astype(BF16).astype(F32)
            if head < 8:
                query[:, head, :] = column
            else:
                fresh[:, head - 8, :] = column
    fresh[:, 2, :] = jnp.broadcast_to(places, (32, 128))

    loads[2].wait()
    loads[3].wait()

    def slots(g, carry):
        first = 8 * g
        score_scale = HD ** (-0.5)
        q = query[pl.ds(first, 8)]
        scores = []
        for i in range(8):
            scores.append(
                lax.dot_general(
                    q[i].astype(BF16),
                    v_keys[first + i],
                    (((1,), (1,)), ((), ())),
                    preferred_element_type=F32,
                )
            )
        scores = jnp.concatenate(scores, axis=0) * score_scale
        new = fresh[pl.ds(first, 8)]
        q = q.reshape(64, HD)

        def spread(i):
            return jnp.broadcast_to(new[:, i : i + 1, :], (8, 8, HD)).reshape(64, HD)

        own = jnp.sum(q * spread(0), axis=1, keepdims=True) * score_scale
        ends = spread(2)[:, 0:1]
        spot = lax.broadcasted_iota(jnp.int32, scores.shape, 1).astype(F32)
        valid = spot < ends
        scores = jnp.where(valid, scores, MASKED)
        peak = jnp.maximum(jnp.max(scores, axis=1, keepdims=True), own)
        probs = jnp.where(valid, jnp.exp(scores - peak), 0.0).astype(BF16).astype(F32)
        own_weight = jnp.exp(own - peak).astype(BF16).astype(F32)
        totals = jnp.sum(probs, axis=1, keepdims=True) + own_weight
        blends = []
        for i in range(8):
            blends.append(
                jnp.dot(
                    probs[8 * i : 8 * (i + 1)].astype(BF16),
                    v_values[first + i],
                    preferred_element_type=F32,
                )
            )
        blend = jnp.concatenate(blends, axis=0) + own_weight * spread(1)
        attended[pl.ds(first, 8)] = (blend / totals).reshape(8, 8, HD)
        return carry

    lax.fori_loop(0, 4, slots, 0)
    for head in range(8):
        h, i = divmod(head, 4)
        abuf[h, rings[h].me, rings[1 - h].me, :, 128 * i : 128 * (i + 1)] = attended[
            :, head, :
        ].astype(BF16)

    a_finish, a_drain = gather_plane(rings, abuf, a_ssem, a_rsem)
    for h in range(2):
        a_finish(h)
        if h == 0:
            loads[4].wait()
        half = abuf.shape[4]
        block = abuf[h].reshape(512, half)
        got = jnp.dot(block, v_out[h * half : (h + 1) * half, :], preferred_element_type=F32)
        acc[h] = got.reshape(4, 4, 32, acc.shape[4])
    total = columns_sum(acc, full, mine, core_in, yring, y_in, y_ssem.at[0], y_rsem.at[0])
    live = as_column(row(live_mask), 64, row0)
    kept = (v_tok[pl.ds(pl.multiple_of(row0, 64), 64), :].astype(F32) + live * total).astype(BF16)

    def r_whole(d):
        return resid.at[d, core]

    def to_core(d):
        send(r_whole(d), r_whole(d), r_ssem.at[1], r_rsem.at[3], {"c": 1 - core})

    resid[yring.me, core] = kept
    gather_direct(yring, r_whole, r_ssem.at[0], lambda i: r_rsem.at[i])
    to_core(yring.me)
    for r in (1, 3, 2):
        wait_bytes(r_whole(yring.places[4 - r]), r_rsem.at[r - 1])
        to_core(yring.places[4 - r])
    wait_bytes(resid.at[:, 1 - core], r_rsem.at[3])

    for a in range(4):
        normed(a, resid[a].astype(F32).reshape(128, depth), row(mlp_gain), sq)
    squares.over_x()
    acc[...] = jnp.zeros_like(acc)
    for load in loads[5:]:
        load.wait()

    s_start1, s_forward1, s_start2, s_forward2, s_finish2 = scatter_stages(
        rings, part, far1, near1, sum1, far2, near2, m_ssem, m_rsem
    )
    g_start1, g_forward1, g_start2, g_forward2, g_finish2, g_drain = gather_stages(
        rings,
        lambda h, k: hid.at[h, k],
        lambda h, k, i: m_ssem.at[k, h, 2 + i],
        lambda h, k, i: m_rsem.at[k, h, 8 + i],
    )

    def compute(k):
        for h in range(2):
            cols = pl.ds(pl.multiple_of((2 * k + h) * cut, 128), cut)
            block = lhs[h].reshape(512, depth)
            for i, v in enumerate((v_gate, v_up)):
                got = jnp.dot(block, v[:, cols], preferred_element_type=F32)
                part[h, k, :, :, :, i * cut : (i + 1) * cut] = got.astype(BF16).reshape(
                    4, 4, 32, cut
                )
        s_start1(k)

    def hidden(k):
        @pl.when(k == 0)
        def _():
            scales[...] = jnp.broadcast_to(squares.scale(), scales.shape)

        scale = scales[:, 0:1]

        def work(direct):
            for h in range(2):
                sums = s_finish2(h, k, direct) * scale
                gate = sums[:, :cut]
                up = sums[:, cut:]
                made = gate * (1.0 / (1.0 + jnp.exp(-gate))) * up
                hid[h, k, rings[h].me, rings[1 - h].me] = made.astype(BF16)

        def go(direct):
            for h in range(2):
                g_start1(h, k, direct)

        either(k, chunks, STRAIGHT[1], work)
        either(k, chunks, STRAIGHT[2], go)

    def down(k):
        g_finish2(k)
        for h in range(2):
            depths = pl.ds(pl.multiple_of((2 * k + h) * cut, 128), cut)
            block = hid[h, k].reshape(512, cut)
            got = jnp.dot(block, v_down[depths, :], preferred_element_type=F32)
            acc[h] += got.reshape(4, 4, 32, acc.shape[4])

    def forward1(k):
        @pl.when(k == 0)
        def _():
            squares.over_z()

        s_forward1(k)

    run_stages(
        chunks,
        (compute, forward1, s_start2, s_forward2, hidden, g_forward1, g_start2, g_forward2, down),
    )

    total = columns_sum(acc, full2, mine2, core_in2, yring, y_in2, y_ssem.at[1], y_rsem.at[1])
    base[...] = kept
    extra[...] = live * total

    squares0.drain()
    squares.drain()
    for h in range(2):
        a_drain(h)
        wait_bytes(q_in1.at[h], q_ssem.at[h, 0])
        wait_bytes(q_in2.at[h], q_ssem.at[h, 1])
    wait_bytes(resid.at[pl.ds(0, 3), 0], r_ssem.at[0])
    wait_bytes(resid.at[:, 0], r_ssem.at[1])

    def drain(k, carry):
        for h in range(2):
            wait_bytes(part.at[h, k, pl.ds(0, 3)], m_ssem.at[k, h, 0])
            wait_bytes(sum1.at[h, k, pl.ds(0, 3)], m_ssem.at[k, h, 1])
            g_drain(h, k)
        return carry

    lax.fori_loop(0, chunks, drain, 0)


def layer_rows(tok, attn_gain, mlp_gain, lengths, live_mask, w_qkv, keys, values, w_out, w_gate, w_up, w_down):
    depth = w_gate.shape[0]
    cut = w_gate.shape[1] // (2 * MLP_CHUNKS)
    half = w_out.shape[0] // 2
    across = w_out.shape[1]
    slots = keys.shape[0]
    q_width = w_qkv.shape[1] // 2
    vmem = pl.BlockSpec(memory_space=pltpu.VMEM)
    hbm = pl.BlockSpec(memory_space=pl.ANY)
    held = (tok, w_qkv, keys, values, w_out, w_gate, w_up, w_down)
    squares = [
        pltpu.VMEM((4, 8, 128), F32),
        pltpu.VMEM((3, 8, 128), F32),
        pltpu.VMEM((8, 128), F32),
        pltpu.VMEM((3, 8, 128), F32),
    ]
    sums = [
        pltpu.VMEM((2, 4, 64, across), BF16),
        pltpu.VMEM((4, 64, across), BF16),
        pltpu.VMEM((4, 64, across), BF16),
        pltpu.VMEM((3, 64, across), BF16),
    ]
    return pl.pallas_call(
        layer_kernel,
        name="layer_rows",
        out_shape=(
            jax.ShapeDtypeStruct((64, across), BF16),
            jax.ShapeDtypeStruct((64, across), F32),
        ),
        in_specs=[hbm] + [vmem] * 4 + [hbm] * 7,
        out_specs=(vmem, vmem),
        scratch_shapes=[
            *[pltpu.VMEM(a.shape, BF16) for a in held],
            pltpu.VMEM((2, 4, 4, 32, q_width), BF16),
            pltpu.VMEM((2, 3, 4, 32, q_width), BF16),
            pltpu.VMEM((2, 4, 32, q_width), BF16),
            pltpu.VMEM((2, 3, 32, q_width), BF16),
            *squares,
            pltpu.VMEM((slots, 8, HD), F32),
            pltpu.VMEM((slots, 8, HD), F32),
            pltpu.VMEM((slots, 8, HD), F32),
            pltpu.VMEM((2, 4, 4, 32, depth), BF16),
            pltpu.VMEM((2, 4, 4, 32, half), BF16),
            pltpu.VMEM((2, 4, 4, 32, across), F32),
            *sums,
            *sums,
            pltpu.VMEM((4, 2, 64, across), BF16),
            *scatter_scratch(MLP_CHUNKS, 2 * cut),
            pltpu.VMEM((2, MLP_CHUNKS, 4, 4, 32, cut), BF16),
            *squares,
            pltpu.VMEM((32, 128), F32),
            pltpu.SemaphoreType.DMA((8,)),
            pltpu.SemaphoreType.DMA((2, 2)),
            pltpu.SemaphoreType.DMA((2, 2)),
            pltpu.SemaphoreType.DMA((4,)),
            pltpu.SemaphoreType.DMA((2,)),
            pltpu.SemaphoreType.DMA((2, 6)),
            pltpu.SemaphoreType.DMA((2, 2)),
            pltpu.SemaphoreType.DMA((2, 5)),
            pltpu.SemaphoreType.DMA((2,)),
            pltpu.SemaphoreType.DMA((4,)),
            pltpu.SemaphoreType.DMA((4,)),
            pltpu.SemaphoreType.DMA((MLP_CHUNKS, 2, 4)),
            pltpu.SemaphoreType.DMA((MLP_CHUNKS, 2, 16)),
        ],
        compiler_params=pltpu.CompilerParams(
            collective_id=0, has_side_effects=True, vmem_limit_bytes=60 * 1024 * 1024
        ),
    )(tok, attn_gain, mlp_gain, lengths, live_mask, w_qkv, keys, values, w_out, w_gate, w_up, w_down)


def per_device(
    tokens,
    attn_gain,
    qkv_weight,
    cache_keys,
    cache_values,
    lengths,
    live_mask,
    out_weight,
    mlp_gain,
    gate_weight,
    up_weight,
    down_weight,
):
    base, extra = layer_rows(
        tokens,
        attn_gain,
        mlp_gain,
        lengths,
        live_mask,
        qkv_weight,
        cache_keys.reshape(cache_keys.shape[0], *cache_keys.shape[2:]),
        cache_values.reshape(cache_values.shape[0], *cache_values.shape[2:]),
        out_weight,
        gate_weight,
        up_weight,
        down_weight,
    )
    return (base.astype(F32) + extra).astype(BF16)


def solution(mesh):
    finer = Mesh(mesh.devices.reshape(4, 4, 4, 2), ("x", "z", "y", "c"))
    return jax.shard_map(
        per_device,
        mesh=finer,
        in_specs=(
            P(None, GX),
            P(GX),
            P(GX, GY),
            P(GX, GY, None, None),
            P(GX, GY, None, None),
            P(),
            P(),
            P(GY, GX),
            P(GX),
            P(GX, GY),
            P(GX, GY),
            P(GY, GX),
        ),
        out_specs=P(GY, GX),
        check_vma=False,
    )
```

```python
import math

import jax
import jax.numpy as jnp
from jax import lax
from jax.experimental import pallas as pl
from jax.experimental.pallas import tpu as pltpu
from jax.sharding import Mesh
from jax.sharding import PartitionSpec as P

D = 8192
HD = 128
GX = ("x", "z")
GY = ("y", "c")
MESH = pl.DeviceIdType.MESH
F32 = jnp.float32
BF16 = jnp.bfloat16

ROPE_BASE = 500000.0
NORM_EPS = 1e-05
MASKED = -1e30

MLP_CHUNKS = 7
STRAIGHT = (0, 0, 0, 0)


def send(src, dst, send_sem, recv_sem, device):
    pltpu.make_async_remote_copy(
        src_ref=src,
        dst_ref=dst,
        send_sem=send_sem,
        recv_sem=recv_sem,
        device_id=device,
        device_id_type=MESH,
    ).start()


def wait_bytes(ref, sem):
    pltpu.make_async_copy(ref, ref, sem).wait()


class Ring:
    def __init__(self, axis):
        self.me = lax.axis_index(axis)
        self.places = [lax.rem(self.me + r, 4) for r in range(4)]
        self.right, self.far, self.left = self.places[1:]
        self.devices = [{axis: place} for place in self.places]
        self.to_right, self.to_far, self.to_left = self.devices[1:]


def scatter_direct(ring, block, into, ssem, rsem):
    for r in (2, 1, 3):
        send(block(ring.places[r]), into(r - 1), ssem, rsem, ring.devices[r])


def gather_direct(ring, whole, ssem, rsem):
    for r in (2, 1, 3):
        send(whole(ring.me), whole(ring.me), ssem, rsem(r - 1), ring.devices[r])


def scatter_start(ring, block, from_far, from_near, ssem, rsem, direct=False):
    if direct:
        for half in range(2):
            send(block(ring.far, half), from_far(half), ssem, rsem(half), ring.to_far)
        for half in range(2):
            send(block(ring.right, half), from_near(0, half), ssem, rsem(2), ring.to_right)
            send(block(ring.left, half), from_near(1, half), ssem, rsem(3), ring.to_left)
        return
    send(block(ring.far, 0), from_far(0), ssem, rsem(0), ring.to_right)
    send(block(ring.far, 1), from_far(1), ssem, rsem(1), ring.to_left)
    send(block(ring.right, 1), from_near(0, 1), ssem, rsem(2), ring.to_right)
    send(block(ring.left, 0), from_near(1, 0), ssem, rsem(3), ring.to_left)


def scatter_forward(ring, block, from_far, from_near, ssem, rsem):
    for way, place, device in ((0, ring.right, ring.to_right), (1, ring.left, ring.to_left)):
        wait_bytes(from_far(way), rsem(way))
        mine = block(place, way)
        mine[...] = (mine[...].astype(F32) + from_far(way)[...].astype(F32)).astype(BF16)
        send(mine, from_near(way, way), ssem, rsem(2 + way), device)


def scatter_finish(own, near, far, rsem):
    total = own.astype(F32)
    if far is not None:
        for way in range(2):
            wait_bytes(far(way), rsem(way))
        total = total + jnp.concatenate([far(0)[...].astype(F32), far(1)[...].astype(F32)], axis=0)
    for way in range(2):
        wait_bytes(near(way), rsem(2 + way))
    return total + near(0)[...].astype(F32) + near(1)[...].astype(F32)


def gather_start(ring, whole, block, ssem, rsem, direct=False):
    if direct:
        for half in range(2):
            send(block(ring.me, half), block(ring.me, half), ssem, rsem(2 + half), ring.to_far)
    send(whole(ring.me), whole(ring.me), ssem, rsem(0), ring.to_right)
    send(whole(ring.me), whole(ring.me), ssem, rsem(1), ring.to_left)


def gather_forward(ring, whole, block, ssem, rsem):
    wait_bytes(whole(ring.left), rsem(0))
    send(block(ring.left, 0), block(ring.left, 0), ssem, rsem(2), ring.to_right)
    wait_bytes(whole(ring.right), rsem(1))
    send(block(ring.right, 1), block(ring.right, 1), ssem, rsem(3), ring.to_left)


def gather_finish(ring, whole, block, rsem, direct=False):
    if direct:
        wait_bytes(whole(ring.left), rsem(0))
        wait_bytes(whole(ring.right), rsem(1))
    wait_bytes(block(ring.far, 0), rsem(2))
    wait_bytes(block(ring.far, 1), rsem(3))


def greet(devices):
    barrier = pltpu.get_barrier_semaphore()
    for device in devices:
        pl.semaphore_signal(barrier, inc=1, device_id=device, device_id_type=MESH)
    return lambda: pl.semaphore_wait(barrier, len(devices))


def row_squares(wide):
    squares = wide * wide
    high = squares.astype(BF16)
    low = (squares - high.astype(F32)).astype(BF16)
    ones = jnp.ones((8, wide.shape[1]), BF16)
    dims = (((1,), (1,)), ((), ()))
    return lax.dot_general(ones, high, dims, preferred_element_type=F32) + lax.dot_general(
        ones, low, dims, preferred_element_type=F32
    )


def as_column(lanes, count, first):
    shape = (count, lanes.shape[1])
    lane = lax.broadcasted_iota(jnp.int32, shape, 1)
    row = lax.broadcasted_iota(jnp.int32, shape, 0)
    return jnp.sum(jnp.where(lane == row + first, lanes, 0.0), axis=1, keepdims=True)


class Squares:
    def __init__(self, rings, sq, sq_x, sq_mid, sq_z, sems):
        self.rings, self.refs, self.sems = rings, (sq, sq_x, sq_mid, sq_z), sems

    def over_x(self):
        sq, sq_x, _, _ = self.refs
        scatter_direct(
            self.rings[0], lambda d: sq.at[d], lambda i: sq_x.at[i], self.sems.at[0], self.sems.at[1]
        )

    def over_z(self):
        sq, sq_x, sq_mid, sq_z = self.refs
        wait_bytes(sq_x, self.sems.at[1])
        sq_mid[...] = sq[self.rings[0].me] + jnp.sum(sq_x[...], axis=0)
        scatter_direct(
            self.rings[1], lambda d: sq_mid, lambda i: sq_z.at[i], self.sems.at[2], self.sems.at[3]
        )

    def scale(self):
        _, _, sq_mid, sq_z = self.refs
        wait_bytes(sq_z, self.sems.at[3])
        total = sq_mid[...] + jnp.sum(sq_z[...], axis=0)
        sums = as_column(total[0:1, :], 32, 32 * self.rings[1].me)
        return lax.rsqrt(sums / D + NORM_EPS)

    def drain(self):
        wait_bytes(self.refs[1], self.sems.at[0])
        wait_bytes(self.refs[3], self.sems.at[2])


def either(k, chunks, straight, work):
    if straight == 0:
        work(False)
        return

    @pl.when(k < chunks - straight)
    def _():
        work(False)

    @pl.when(k >= chunks - straight)
    def _():
        work(True)


def run_stages(count, stages):
    def body(t, carry):
        for lag, stage in enumerate(stages):
            k = t - 2 * lag

            @pl.when((k >= 0) & (k < count))
            def _():
                stage(k)

        return carry

    lax.fori_loop(0, count + 2 * len(stages) - 2, body, 0)


def scatter_stages(rings, part, far1, near1, sum1, far2, near2, ssem, rsem):
    def block1(h, k):
        return lambda d, half: part.at[h, k, d, pl.ds(2 * half, 2)]

    def far_in1(h, k):
        return lambda way: far1.at[h, k, way]

    def near_in1(h, k):
        return lambda way, half: near1.at[h, k, way, pl.ds(2 * half, 2)]

    def block2(h, k):
        return lambda d, half: sum1.at[h, k, d, pl.ds(16 * half, 16)]

    def far_in2(h, k):
        return lambda way: far2.at[h, k, way]

    def near_in2(h, k):
        return lambda way, half: near2.at[h, k, way, pl.ds(16 * half, 16)]

    def rs(h, k, base):
        return lambda i: rsem.at[k, h, base + i]

    chunks = part.shape[1]

    def start1(h, k):
        def work(direct):
            refs = (block1(h, k), far_in1(h, k), near_in1(h, k))
            scatter_start(rings[h], *refs, ssem.at[k, h, 0], rs(h, k, 0), direct)

        either(k, chunks, STRAIGHT[0], work)

    def forward1(k):
        @pl.when(k < chunks - STRAIGHT[0])
        def _():
            for h in range(2):
                refs = (block1(h, k), far_in1(h, k), near_in1(h, k))
                scatter_forward(rings[h], *refs, ssem.at[k, h, 0], rs(h, k, 0))

    def start2(k):
        def total(direct):
            for h in range(2):
                own = part[h, k, rings[h].me]
                far = far_in1(h, k) if direct else None
                got = scatter_finish(own, lambda way: near1.at[h, k, way], far, rs(h, k, 0))
                sum1[h, k] = got.astype(BF16)

        def work(direct):
            for h in range(2):
                refs = (block2(h, k), far_in2(h, k), near_in2(h, k))
                scatter_start(rings[1 - h], *refs, ssem.at[k, h, 1], rs(h, k, 4), direct)

        either(k, chunks, STRAIGHT[0], total)
        either(k, chunks, STRAIGHT[1], work)

    def forward2(k):
        @pl.when(k < chunks - STRAIGHT[1])
        def _():
            for h in range(2):
                refs = (block2(h, k), far_in2(h, k), near_in2(h, k))
                scatter_forward(rings[1 - h], *refs, ssem.at[k, h, 1], rs(h, k, 4))

    def finish2(h, k, direct):
        own = sum1[h, k, rings[1 - h].me]
        far = far_in2(h, k) if direct else None
        return scatter_finish(own, lambda way: near2.at[h, k, way], far, rs(h, k, 4))

    return start1, forward1, start2, forward2, finish2


def scatter_scratch(chunks, width):
    return [
        pltpu.VMEM((2, chunks, 4, 4, 32, width), BF16),
        pltpu.VMEM((2, chunks, 2, 2, 32, width), BF16),
        pltpu.VMEM((2, chunks, 2, 4, 32, width), BF16),
        pltpu.VMEM((2, chunks, 4, 32, width), BF16),
        pltpu.VMEM((2, chunks, 2, 16, width), BF16),
        pltpu.VMEM((2, chunks, 2, 32, width), BF16),
    ]


def gather_stages(rings, buf, ssem, rsem):
    def inner(h, k):
        ring = rings[1 - h]
        row = rings[h].me
        return (
            ring,
            lambda d: buf(h, k).at[row, d],
            lambda d, half: buf(h, k).at[row, d, pl.ds(16 * half, 16)],
        )

    def outer(h, k):
        return (
            rings[h],
            lambda d: buf(h, k).at[d],
            lambda d, half: buf(h, k).at[d, pl.ds(2 * half, 2)],
        )

    chunks = MLP_CHUNKS

    def start1(h, k, direct):
        ring, whole, block = inner(h, k)
        gather_start(ring, whole, block, ssem(h, k, 0), lambda i: rsem(h, k, i), direct)

    def forward1(k):
        @pl.when(k < chunks - STRAIGHT[2])
        def _():
            for h in range(2):
                ring, whole, block = inner(h, k)
                gather_forward(ring, whole, block, ssem(h, k, 0), lambda i: rsem(h, k, i))

    def start2(k):
        def finish(direct):
            for h in range(2):
                ring, whole, block = inner(h, k)
                gather_finish(ring, whole, block, lambda i: rsem(h, k, i), direct)

        def work(direct):
            for h in range(2):
                ring, whole, block = outer(h, k)
                gather_start(ring, whole, block, ssem(h, k, 1), lambda i: rsem(h, k, 4 + i), direct)

        either(k, chunks, STRAIGHT[2], finish)
        either(k, chunks, STRAIGHT[3], work)

    def forward2(k):
        @pl.when(k < chunks - STRAIGHT[3])
        def _():
            for h in range(2):
                ring, whole, block = outer(h, k)
                gather_forward(ring, whole, block, ssem(h, k, 1), lambda i: rsem(h, k, 4 + i))

    def finish2(k):
        def finish(direct):
            for h in range(2):
                ring, whole, block = outer(h, k)
                gather_finish(ring, whole, block, lambda i: rsem(h, k, 4 + i), direct)

        either(k, chunks, STRAIGHT[3], finish)

    def drain(h, k):
        wait_bytes(buf(h, k).at[0, pl.ds(0, 3)], ssem(h, k, 0))
        wait_bytes(buf(h, k).at[pl.ds(0, 3)], ssem(h, k, 1))

    return start1, forward1, start2, forward2, finish2, drain


def columns_sum(acc, full, mine, core_in, ring, y_in, ssem, rsem):
    core = lax.axis_index("c")

    def made(c, y):
        rows = []
        for i in range(2):
            z = 2 * c + i
            rows.append(acc[0, y, z] + acc[1, z, y])
        return jnp.concatenate(rows, axis=0)

    for r in (2, 1, 3, 0):
        place = ring.places[r]
        full[place] = made(1 - core, place).astype(BF16)
        send(full.at[place], core_in.at[place], ssem.at[0], rsem.at[r], {"c": 1 - core})
    for r in (2, 1, 3, 0):
        place = ring.places[r]
        both = made(core, place)
        wait_bytes(core_in.at[place], rsem.at[r])
        both = both + core_in[place].astype(F32)
        if r == 0:
            total = both
        else:
            mine[place] = both.astype(BF16)
            send(mine.at[place], y_in.at[r - 1], ssem.at[1], rsem.at[4], ring.devices[r])
    wait_bytes(y_in, rsem.at[4])
    total = total + jnp.sum(y_in[...].astype(F32), axis=0)
    wait_bytes(core_in, ssem.at[0])
    wait_bytes(y_in, ssem.at[1])
    return total


class PlaneGather:
    def __init__(self, rings, buf, ssem, rsem):
        self.rings, self.buf, self.ssem, self.rsem = rings, buf, ssem, rsem

    def block(self, h, r, piece):
        place = self.rings[1 - h].places[r]
        return self.buf.at[h, self.rings[h].me, place, pl.ds(16 * piece, 16)]

    def outward(self, h, r, piece):
        ref = self.block(h, r, piece)
        for way in (2, 1, 3):
            device = self.rings[h].devices[way]
            send(ref, ref, self.ssem.at[h, piece], self.rsem.at[h, piece, 2 + way], device)

    def start(self, piece):
        for h in range(2):
            ref = self.block(h, 0, piece)
            for way in (2, 1, 3):
                device = self.rings[1 - h].devices[way]
                send(ref, ref, self.ssem.at[h, piece], self.rsem.at[h, piece, way - 1], device)
        for h in range(2):
            self.outward(h, 0, piece)

    def relay(self, piece):
        for way in (1, 3, 2):
            for h in range(2):
                wait_bytes(self.block(h, 4 - way, piece), self.rsem.at[h, piece, way - 1])
                self.outward(h, 4 - way, piece)

    def finish(self, h, way, piece):
        place = self.rings[h].places[4 - way]
        wait_bytes(self.buf.at[h, place, :, pl.ds(16 * piece, 16)], self.rsem.at[h, piece, 2 + way])

    def drain(self):
        for h in range(2):
            for piece in range(2):
                wait_bytes(self.buf.at[h, 0, pl.ds(0, 3), pl.ds(0, 16)], self.ssem.at[h, piece])
                wait_bytes(self.buf.at[h, pl.ds(0, 3), :, pl.ds(0, 16)], self.ssem.at[h, piece])


def rotation(places):
    lane = lax.broadcasted_iota(jnp.int32, (1, HD), 1)
    index = lax.rem(lane, HD // 2).astype(F32)
    inv_freq = jnp.exp(index * (-2.0 * math.log(ROPE_BASE) / HD))
    angles = places * inv_freq
    sine = jnp.sin(angles)
    return jnp.cos(angles), jnp.where(lane < HD // 2, -sine, sine)


def layer_kernel(
    tok,
    attn_gain,
    mlp_gain,
    lengths,
    live_mask,
    w_qkv,
    keys,
    values,
    w_out,
    w_gate,
    w_up,
    w_down,
    base,
    extra,
    v_tok,
    v_qkv,
    v_keys,
    v_values,
    v_out,
    v_gate,
    v_up,
    v_down,
    qa_part,
    qa_in1,
    qa_sum1,
    qa_in2,
    qb_part,
    qb_in1,
    qb_sum1,
    qb_in2,
    sq0,
    sq0_x,
    sq0_mid,
    sq0_z,
    query,
    fresh,
    attended,
    lhs,
    abuf,
    acc,
    full,
    mine,
    core_in,
    y_in,
    full2,
    mine2,
    core_in2,
    y_in2,
    resid,
    part,
    far1,
    near1,
    sum1,
    far2,
    near2,
    hid,
    sq,
    sq_x,
    sq_mid,
    sq_z,
    scales,
    wsem,
    q_ssem,
    q_rsem,
    sqs0,
    a_ssem,
    a_rsem,
    y_ssem,
    y_rsem,
    r_ssem,
    r_rsem,
    sqs,
    m_ssem,
    m_rsem,
):
    rings = (Ring("x"), Ring("z"))
    yring = Ring("y")
    core = lax.axis_index("c")
    chunks, width = part.shape[1], part.shape[5]
    cut = width // 2
    depth = lhs.shape[4]
    slot0 = 32 * (4 * rings[0].me + rings[1].me)
    row0 = 64 * (2 * yring.me + core)
    loads = [
        pltpu.make_async_copy(src, dst, wsem.at[i])
        for i, (src, dst) in enumerate(
            (
                (tok, v_tok),
                (w_qkv, v_qkv),
                (keys, v_keys),
                (values, v_values),
                (w_out, v_out),
                (w_gate, v_gate),
                (w_up, v_up),
                (w_down, v_down),
            )
        )
    ]
    loads[0].start()
    loads[1].start()
    met = greet(
        [*rings[0].devices[1:], *rings[1].devices[1:], *yring.devices[1:], {"c": 1 - core}]
    )

    def row(ref):
        return ref[...].astype(F32).reshape(1, ref.shape[0])

    def normed(a, wide, gain):
        scaled = (wide * gain).astype(BF16).reshape(4, 32, depth)
        lhs[0, a] = scaled
        for b in range(4):
            lhs[1, b, a] = scaled[b]

    loads[0].wait()
    for a in range(4):
        normed(a, v_tok[128 * a : 128 * (a + 1), :].astype(F32), row(attn_gain))
    loads[1].wait()
    for load in loads[2:]:
        load.start()
    squares0 = Squares(rings, sq0, sq0_x, sq0_mid, sq0_z, sqs0)
    squares = Squares(rings, sq, sq_x, sq_mid, sq_z, sqs)
    pieces = (
        (qa_part, qa_in1, qa_sum1, qa_in2, 0, 3),
        (qb_part, qb_in1, qb_sum1, qb_in2, 3, 5),
    )
    for p, (q_part, q_in1, _, _, begin, end) in enumerate(pieces):
        width_q = HD * (end - begin)
        for h in range(2):
            columns = slice(HD * (5 * h + begin), HD * (5 * h + end))
            got = jnp.dot(lhs[h].reshape(512, depth), v_qkv[:, columns], preferred_element_type=F32)
            q_part[h] = got.astype(BF16).reshape(4, 4, 32, width_q)
            if p == 0 and h == 0:
                met()
            scatter_direct(
                rings[h],
                lambda d: q_part.at[h, d],
                lambda i: q_in1.at[h, i],
                q_ssem.at[p, h, 0],
                q_rsem.at[p, h, 0],
            )
    for a in range(4):
        sq0[a] = row_squares(v_tok[128 * a : 128 * (a + 1), :].astype(F32))
    squares0.over_x()
    places = as_column(row(lengths), 32, slot0)
    cosine, sine = rotation(places)
    fresh[:, 2, :] = jnp.broadcast_to(places, (32, 128))
    for p, (q_part, q_in1, q_sum1, q_in2, _, _) in enumerate(pieces):
        for h in range(2):
            wait_bytes(q_in1.at[h], q_rsem.at[p, h, 0])
            total = q_part[h, rings[h].me].astype(F32)
            for i in range(3):
                total = total + q_in1[h, i].astype(F32)
            q_sum1[h] = total.astype(BF16)
            scatter_direct(
                rings[1 - h],
                lambda d: q_sum1.at[h, d],
                lambda i: q_in2.at[h, i],
                q_ssem.at[p, h, 1],
                q_rsem.at[p, h, 1],
            )
        if p == 0:
            squares0.over_z()
    scale = squares0.scale()
    for p, (_, _, q_sum1, q_in2, begin, end) in enumerate(pieces):
        for h in range(2):
            wait_bytes(q_in2.at[h], q_rsem.at[p, h, 1])
            total = q_sum1[h, rings[1 - h].me].astype(F32)
            for i in range(3):
                total = total + q_in2[h, i].astype(F32)
            sums = total * scale
            for i in range(end - begin):
                column = sums[:, 128 * i : 128 * (i + 1)]
                head = 5 * h + begin + i
                if head < 9:
                    column = column * cosine + pltpu.roll(column, HD // 2, 1) * sine
                column = column.astype(BF16).astype(F32)
                if head < 8:
                    query[:, head, :] = column
                else:
                    fresh[:, head - 8, :] = column

    loads[2].wait()
    loads[3].wait()

    def slots(g, carry):
        first = 8 * g
        score_scale = HD ** (-0.5)
        q = query[pl.ds(first, 8)]
        scores = []
        for i in range(8):
            scores.append(
                lax.dot_general(
                    q[i].astype(BF16),
                    v_keys[first + i],
                    (((1,), (1,)), ((), ())),
                    preferred_element_type=F32,
                )
            )
        scores = jnp.concatenate(scores, axis=0) * score_scale
        new = fresh[pl.ds(first, 8)]
        q = q.reshape(64, HD)

        def spread(i):
            return jnp.broadcast_to(new[:, i : i + 1, :], (8, 8, HD)).reshape(64, HD)

        own = jnp.sum(q * spread(0), axis=1, keepdims=True) * score_scale
        ends = spread(2)[:, 0:1]
        spot = lax.broadcasted_iota(jnp.int32, scores.shape, 1).astype(F32)
        valid = spot < ends
        scores = jnp.where(valid, scores, MASKED)
        peak = jnp.maximum(jnp.max(scores, axis=1, keepdims=True), own)
        probs = jnp.where(valid, jnp.exp(scores - peak), 0.0).astype(BF16).astype(F32)
        own_weight = jnp.exp(own - peak).astype(BF16).astype(F32)
        totals = jnp.sum(probs, axis=1, keepdims=True) + own_weight
        blends = []
        for i in range(8):
            blends.append(
                jnp.dot(
                    probs[8 * i : 8 * (i + 1)].astype(BF16),
                    v_values[first + i],
                    preferred_element_type=F32,
                )
            )
        blend = jnp.concatenate(blends, axis=0) + own_weight * spread(1)
        attended[pl.ds(first, 8)] = (blend / totals).reshape(8, 8, HD)
        return carry

    gather = PlaneGather(rings, abuf, a_ssem, a_rsem)
    for piece in range(2):
        lax.fori_loop(2 * piece, 2 * piece + 2, slots, 0)
        rows = pl.ds(16 * piece, 16)
        for head in range(8):
            h, i = divmod(head, 4)
            abuf[h, rings[h].me, rings[1 - h].me, rows, 128 * i : 128 * (i + 1)] = attended[
                rows, head, :
            ].astype(BF16)
        gather.start(piece)
    for piece in range(2):
        gather.relay(piece)
    half = abuf.shape[4]
    loads[4].wait()
    for h in range(2):
        for piece in range(2):
            for way in (1, 3, 2):
                gather.finish(h, way, piece)
        block = abuf[h].reshape(512, half)
        got = jnp.dot(block, v_out[h * half : (h + 1) * half, :], preferred_element_type=F32)
        acc[h] = got.reshape(4, 4, 32, acc.shape[4])
    total = columns_sum(acc, full, mine, core_in, yring, y_in, y_ssem.at[0], y_rsem.at[0])
    live = as_column(row(live_mask), 64, row0)
    kept = (v_tok[pl.ds(pl.multiple_of(row0, 64), 64), :].astype(F32) + live * total).astype(BF16)

    def r_whole(d):
        return resid.at[d, core]

    def to_core(r):
        ref = r_whole(yring.places[r])
        send(ref, ref, r_ssem.at[1], r_rsem.at[3 + r], {"c": 1 - core})

    def take(r):
        place = yring.places[r]
        wait_bytes(resid.at[place, 1 - core], r_rsem.at[3 + r])
        normed(place, resid[place].astype(F32).reshape(128, depth), row(mlp_gain))

    resid[yring.me, core] = kept
    gather_direct(yring, r_whole, r_ssem.at[0], lambda i: r_rsem.at[i])
    to_core(0)
    acc[...] = jnp.zeros_like(acc)
    take(0)
    for r in (1, 3, 2):
        wait_bytes(r_whole(yring.places[4 - r]), r_rsem.at[r - 1])
        to_core(4 - r)
    for r in (1, 3, 2):
        take(4 - r)
    for load in loads[5:]:
        load.wait()

    s_start1, s_forward1, s_start2, s_forward2, s_finish2 = scatter_stages(
        rings, part, far1, near1, sum1, far2, near2, m_ssem, m_rsem
    )
    g_start1, g_forward1, g_start2, g_forward2, g_finish2, g_drain = gather_stages(
        rings,
        lambda h, k: hid.at[h, k],
        lambda h, k, i: m_ssem.at[k, h, 2 + i],
        lambda h, k, i: m_rsem.at[k, h, 8 + i],
    )

    def compute(k):
        for h in range(2):
            cols = pl.ds(pl.multiple_of((2 * k + h) * cut, 128), cut)
            block = lhs[h].reshape(512, depth)
            for i, v in enumerate((v_gate, v_up)):
                got = jnp.dot(block, v[:, cols], preferred_element_type=F32)
                part[h, k, :, :, :, i * cut : (i + 1) * cut] = got.astype(BF16).reshape(
                    4, 4, 32, cut
                )
            s_start1(h, k)

        @pl.when(k == 0)
        def _():
            for a in range(4):
                sq[a] = row_squares(resid[a].astype(F32).reshape(128, depth))
            squares.over_x()

    def hidden(k):
        @pl.when(k == 0)
        def _():
            scales[...] = jnp.broadcast_to(squares.scale(), scales.shape)

        scale = scales[:, 0:1]

        def work(direct):
            for h in range(2):
                sums = s_finish2(h, k, direct) * scale
                gate = sums[:, :cut]
                up = sums[:, cut:]
                made = gate * (1.0 / (1.0 + jnp.exp(-gate))) * up
                hid[h, k, rings[h].me, rings[1 - h].me] = made.astype(BF16)

        def go(direct):
            for h in range(2):
                g_start1(h, k, direct)

        either(k, chunks, STRAIGHT[1], work)
        either(k, chunks, STRAIGHT[2], go)

    def down(k):
        g_finish2(k)
        for h in range(2):
            depths = pl.ds(pl.multiple_of((2 * k + h) * cut, 128), cut)
            block = hid[h, k].reshape(512, cut)
            got = jnp.dot(block, v_down[depths, :], preferred_element_type=F32)
            acc[h] += got.reshape(4, 4, 32, acc.shape[4])

    def forward1(k):
        @pl.when(k == 0)
        def _():
            squares.over_z()

        s_forward1(k)

    run_stages(
        chunks,
        (compute, forward1, s_start2, s_forward2, hidden, g_forward1, g_start2, g_forward2, down),
    )

    total = columns_sum(acc, full2, mine2, core_in2, yring, y_in2, y_ssem.at[1], y_rsem.at[1])
    base[...] = kept
    extra[...] = live * total

    squares0.drain()
    squares.drain()
    gather.drain()
    for p, (_, q_in1, _, q_in2, _, _) in enumerate(pieces):
        for h in range(2):
            wait_bytes(q_in1.at[h], q_ssem.at[p, h, 0])
            wait_bytes(q_in2.at[h], q_ssem.at[p, h, 1])
    wait_bytes(resid.at[pl.ds(0, 3), 0], r_ssem.at[0])
    wait_bytes(resid.at[:, 0], r_ssem.at[1])

    def drain(k, carry):
        for h in range(2):
            wait_bytes(part.at[h, k, pl.ds(0, 3)], m_ssem.at[k, h, 0])
            wait_bytes(sum1.at[h, k, pl.ds(0, 3)], m_ssem.at[k, h, 1])
            g_drain(h, k)
        return carry

    lax.fori_loop(0, chunks, drain, 0)


def q_scratch(width):
    return [
        pltpu.VMEM((2, 4, 4, 32, width), BF16),
        pltpu.VMEM((2, 3, 4, 32, width), BF16),
        pltpu.VMEM((2, 4, 32, width), BF16),
        pltpu.VMEM((2, 3, 32, width), BF16),
    ]


def layer_rows(tok, attn_gain, mlp_gain, lengths, live_mask, w_qkv, keys, values, w_out, w_gate, w_up, w_down):
    depth = w_gate.shape[0]
    cut = w_gate.shape[1] // (2 * MLP_CHUNKS)
    half = w_out.shape[0] // 2
    across = w_out.shape[1]
    slots = keys.shape[0]
    vmem = pl.BlockSpec(memory_space=pltpu.VMEM)
    hbm = pl.BlockSpec(memory_space=pl.ANY)
    held = (tok, w_qkv, keys, values, w_out, w_gate, w_up, w_down)
    squares = [
        pltpu.VMEM((4, 8, 128), F32),
        pltpu.VMEM((3, 8, 128), F32),
        pltpu.VMEM((8, 128), F32),
        pltpu.VMEM((3, 8, 128), F32),
    ]
    sums = [
        pltpu.VMEM((4, 64, across), BF16),
        pltpu.VMEM((4, 64, across), BF16),
        pltpu.VMEM((4, 64, across), BF16),
        pltpu.VMEM((3, 64, across), BF16),
    ]
    return pl.pallas_call(
        layer_kernel,
        name="layer_rows",
        out_shape=(
            jax.ShapeDtypeStruct((64, across), BF16),
            jax.ShapeDtypeStruct((64, across), F32),
        ),
        in_specs=[hbm] + [vmem] * 4 + [hbm] * 7,
        out_specs=(vmem, vmem),
        scratch_shapes=[
            *[pltpu.VMEM(a.shape, BF16) for a in held],
            *q_scratch(3 * HD),
            *q_scratch(2 * HD),
            *squares,
            pltpu.VMEM((slots, 8, HD), F32),
            pltpu.VMEM((slots, 8, HD), F32),
            pltpu.VMEM((slots, 8, HD), F32),
            pltpu.VMEM((2, 4, 4, 32, depth), BF16),
            pltpu.VMEM((2, 4, 4, 32, half), BF16),
            pltpu.VMEM((2, 4, 4, 32, across), F32),
            *sums,
            *sums,
            pltpu.VMEM((4, 2, 64, across), BF16),
            *scatter_scratch(MLP_CHUNKS, 2 * cut),
            pltpu.VMEM((2, MLP_CHUNKS, 4, 4, 32, cut), BF16),
            *squares,
            pltpu.VMEM((32, 128), F32),
            pltpu.SemaphoreType.DMA((8,)),
            pltpu.SemaphoreType.DMA((2, 2, 2)),
            pltpu.SemaphoreType.DMA((2, 2, 2)),
            pltpu.SemaphoreType.DMA((4,)),
            pltpu.SemaphoreType.DMA((2, 2)),
            pltpu.SemaphoreType.DMA((2, 2, 6)),
            pltpu.SemaphoreType.DMA((2, 2)),
            pltpu.SemaphoreType.DMA((2, 5)),
            pltpu.SemaphoreType.DMA((2,)),
            pltpu.SemaphoreType.DMA((7,)),
            pltpu.SemaphoreType.DMA((4,)),
            pltpu.SemaphoreType.DMA((MLP_CHUNKS, 2, 4)),
            pltpu.SemaphoreType.DMA((MLP_CHUNKS, 2, 16)),
        ],
        compiler_params=pltpu.CompilerParams(
            collective_id=0, has_side_effects=True, vmem_limit_bytes=60 * 1024 * 1024
        ),
    )(tok, attn_gain, mlp_gain, lengths, live_mask, w_qkv, keys, values, w_out, w_gate, w_up, w_down)


def per_device(
    tokens,
    attn_gain,
    qkv_weight,
    cache_keys,
    cache_values,
    lengths,
    live_mask,
    out_weight,
    mlp_gain,
    gate_weight,
    up_weight,
    down_weight,
):
    base, extra = layer_rows(
        tokens,
        attn_gain,
        mlp_gain,
        lengths,
        live_mask,
        qkv_weight,
        cache_keys.reshape(cache_keys.shape[0], *cache_keys.shape[2:]),
        cache_values.reshape(cache_values.shape[0], *cache_values.shape[2:]),
        out_weight,
        gate_weight,
        up_weight,
        down_weight,
    )
    return (base.astype(F32) + extra).astype(BF16)


def solution(mesh):
    finer = Mesh(mesh.devices.reshape(4, 4, 4, 2), ("x", "z", "y", "c"))
    return jax.shard_map(
        per_device,
        mesh=finer,
        in_specs=(
            P(None, GX),
            P(GX),
            P(GX, GY),
            P(GX, GY, None, None),
            P(GX, GY, None, None),
            P(),
            P(),
            P(GY, GX),
            P(GX),
            P(GX, GY),
            P(GX, GY),
            P(GY, GX),
        ),
        out_specs=P(GY, GX),
        check_vma=False,
    )
```

```python
import math

import jax
import jax.numpy as jnp
from jax import lax
from jax.experimental import pallas as pl
from jax.experimental.pallas import tpu as pltpu
from jax.sharding import Mesh
from jax.sharding import PartitionSpec as P

D = 8192
HD = 128
GX = ("x", "z")
GY = ("y", "c")
MESH = pl.DeviceIdType.MESH
F32 = jnp.float32
BF16 = jnp.bfloat16

ROPE_BASE = 500000.0
NORM_EPS = 1e-05
MASKED = -1e30

MLP_CHUNKS = 7
STRAIGHT = (0, 0, 0, 0)


def send(src, dst, send_sem, recv_sem, device):
    pltpu.make_async_remote_copy(
        src_ref=src,
        dst_ref=dst,
        send_sem=send_sem,
        recv_sem=recv_sem,
        device_id=device,
        device_id_type=MESH,
    ).start()


def wait_bytes(ref, sem):
    pltpu.make_async_copy(ref, ref, sem).wait()


class Ring:
    def __init__(self, axis):
        self.me = lax.axis_index(axis)
        self.places = [lax.rem(self.me + r, 4) for r in range(4)]
        self.right, self.far, self.left = self.places[1:]
        self.devices = [{axis: place} for place in self.places]
        self.to_right, self.to_far, self.to_left = self.devices[1:]


def scatter_direct(ring, block, into, ssem, rsem):
    for r in (2, 1, 3):
        send(block(ring.places[r]), into(r - 1), ssem, rsem, ring.devices[r])


def gather_direct(ring, whole, ssem, rsem):
    for r in (2, 1, 3):
        send(whole(ring.me), whole(ring.me), ssem, rsem(r - 1), ring.devices[r])


def scatter_start(ring, block, from_far, from_near, ssem, rsem, direct=False):
    if direct:
        for half in range(2):
            send(block(ring.far, half), from_far(half), ssem, rsem(half), ring.to_far)
        for half in range(2):
            send(block(ring.right, half), from_near(0, half), ssem, rsem(2), ring.to_right)
            send(block(ring.left, half), from_near(1, half), ssem, rsem(3), ring.to_left)
        return
    send(block(ring.far, 0), from_far(0), ssem, rsem(0), ring.to_right)
    send(block(ring.far, 1), from_far(1), ssem, rsem(1), ring.to_left)
    send(block(ring.right, 1), from_near(0, 1), ssem, rsem(2), ring.to_right)
    send(block(ring.left, 0), from_near(1, 0), ssem, rsem(3), ring.to_left)


def scatter_forward(ring, block, from_far, from_near, ssem, rsem):
    for way, place, device in ((0, ring.right, ring.to_right), (1, ring.left, ring.to_left)):
        wait_bytes(from_far(way), rsem(way))
        mine = block(place, way)
        mine[...] = (mine[...].astype(F32) + from_far(way)[...].astype(F32)).astype(BF16)
        send(mine, from_near(way, way), ssem, rsem(2 + way), device)


def scatter_finish(own, near, far, rsem):
    total = own.astype(F32)
    if far is not None:
        for way in range(2):
            wait_bytes(far(way), rsem(way))
        total = total + jnp.concatenate([far(0)[...].astype(F32), far(1)[...].astype(F32)], axis=0)
    for way in range(2):
        wait_bytes(near(way), rsem(2 + way))
    return total + near(0)[...].astype(F32) + near(1)[...].astype(F32)


def gather_start(ring, whole, block, ssem, rsem, direct=False):
    if direct:
        for half in range(2):
            send(block(ring.me, half), block(ring.me, half), ssem, rsem(2 + half), ring.to_far)
    send(whole(ring.me), whole(ring.me), ssem, rsem(0), ring.to_right)
    send(whole(ring.me), whole(ring.me), ssem, rsem(1), ring.to_left)


def gather_forward(ring, whole, block, ssem, rsem):
    wait_bytes(whole(ring.left), rsem(0))
    send(block(ring.left, 0), block(ring.left, 0), ssem, rsem(2), ring.to_right)
    wait_bytes(whole(ring.right), rsem(1))
    send(block(ring.right, 1), block(ring.right, 1), ssem, rsem(3), ring.to_left)


def gather_finish(ring, whole, block, rsem, direct=False):
    if direct:
        wait_bytes(whole(ring.left), rsem(0))
        wait_bytes(whole(ring.right), rsem(1))
    wait_bytes(block(ring.far, 0), rsem(2))
    wait_bytes(block(ring.far, 1), rsem(3))


def greet(devices):
    barrier = pltpu.get_barrier_semaphore()
    for device in devices:
        pl.semaphore_signal(barrier, inc=1, device_id=device, device_id_type=MESH)
    return lambda: pl.semaphore_wait(barrier, len(devices))


def row_squares(wide):
    squares = wide * wide
    high = squares.astype(BF16)
    low = (squares - high.astype(F32)).astype(BF16)
    ones = jnp.ones((8, wide.shape[1]), BF16)
    dims = (((1,), (1,)), ((), ()))
    return lax.dot_general(ones, high, dims, preferred_element_type=F32) + lax.dot_general(
        ones, low, dims, preferred_element_type=F32
    )


def as_column(lanes, count, first):
    shape = (count, lanes.shape[1])
    lane = lax.broadcasted_iota(jnp.int32, shape, 1)
    row = lax.broadcasted_iota(jnp.int32, shape, 0)
    return jnp.sum(jnp.where(lane == row + first, lanes, 0.0), axis=1, keepdims=True)


class Squares:
    def __init__(self, rings, sq, sq_x, sq_mid, sq_z, sems):
        self.rings, self.refs, self.sems = rings, (sq, sq_x, sq_mid, sq_z), sems

    def over_x(self):
        sq, sq_x, _, _ = self.refs
        scatter_direct(
            self.rings[0], lambda d: sq.at[d], lambda i: sq_x.at[i], self.sems.at[0], self.sems.at[1]
        )

    def over_z(self):
        sq, sq_x, sq_mid, sq_z = self.refs
        wait_bytes(sq_x, self.sems.at[1])
        sq_mid[...] = sq[self.rings[0].me] + jnp.sum(sq_x[...], axis=0)
        scatter_direct(
            self.rings[1], lambda d: sq_mid, lambda i: sq_z.at[i], self.sems.at[2], self.sems.at[3]
        )

    def scale(self):
        _, _, sq_mid, sq_z = self.refs
        wait_bytes(sq_z, self.sems.at[3])
        total = sq_mid[...] + jnp.sum(sq_z[...], axis=0)
        sums = as_column(total[0:1, :], 32, 32 * self.rings[1].me)
        return lax.rsqrt(sums / D + NORM_EPS)

    def drain(self):
        wait_bytes(self.refs[1], self.sems.at[0])
        wait_bytes(self.refs[3], self.sems.at[2])


def either(k, chunks, straight, work):
    if straight == 0:
        work(False)
        return

    @pl.when(k < chunks - straight)
    def _():
        work(False)

    @pl.when(k >= chunks - straight)
    def _():
        work(True)


def run_stages(count, stages):
    def body(t, carry):
        for lag, stage in enumerate(stages):
            k = t - 2 * lag

            @pl.when((k >= 0) & (k < count))
            def _():
                stage(k)

        return carry

    lax.fori_loop(0, count + 2 * len(stages) - 2, body, 0)


def scatter_stages(rings, part, far1, near1, sum1, far2, near2, ssem, rsem):
    def block1(h, k):
        return lambda d, half: part.at[h, k, d, pl.ds(2 * half, 2)]

    def far_in1(h, k):
        return lambda way: far1.at[h, k, way]

    def near_in1(h, k):
        return lambda way, half: near1.at[h, k, way, pl.ds(2 * half, 2)]

    def block2(h, k):
        return lambda d, half: sum1.at[h, k, d, pl.ds(16 * half, 16)]

    def far_in2(h, k):
        return lambda way: far2.at[h, k, way]

    def near_in2(h, k):
        return lambda way, half: near2.at[h, k, way, pl.ds(16 * half, 16)]

    def rs(h, k, base):
        return lambda i: rsem.at[k, h, base + i]

    chunks = part.shape[1]

    def start1(h, k):
        def work(direct):
            refs = (block1(h, k), far_in1(h, k), near_in1(h, k))
            scatter_start(rings[h], *refs, ssem.at[k, h, 0], rs(h, k, 0), direct)

        either(k, chunks, STRAIGHT[0], work)

    def forward1(k):
        @pl.when(k < chunks - STRAIGHT[0])
        def _():
            for h in range(2):
                refs = (block1(h, k), far_in1(h, k), near_in1(h, k))
                scatter_forward(rings[h], *refs, ssem.at[k, h, 0], rs(h, k, 0))

    def start2(k):
        def total(direct):
            for h in range(2):
                own = part[h, k, rings[h].me]
                far = far_in1(h, k) if direct else None
                got = scatter_finish(own, lambda way: near1.at[h, k, way], far, rs(h, k, 0))
                sum1[h, k] = got.astype(BF16)

        def work(direct):
            for h in range(2):
                refs = (block2(h, k), far_in2(h, k), near_in2(h, k))
                scatter_start(rings[1 - h], *refs, ssem.at[k, h, 1], rs(h, k, 4), direct)

        either(k, chunks, STRAIGHT[0], total)
        either(k, chunks, STRAIGHT[1], work)

    def forward2(k):
        @pl.when(k < chunks - STRAIGHT[1])
        def _():
            for h in range(2):
                refs = (block2(h, k), far_in2(h, k), near_in2(h, k))
                scatter_forward(rings[1 - h], *refs, ssem.at[k, h, 1], rs(h, k, 4))

    def finish2(h, k, direct):
        own = sum1[h, k, rings[1 - h].me]
        far = far_in2(h, k) if direct else None
        return scatter_finish(own, lambda way: near2.at[h, k, way], far, rs(h, k, 4))

    return start1, forward1, start2, forward2, finish2


def scatter_scratch(chunks, width):
    return [
        pltpu.VMEM((2, chunks, 4, 4, 32, width), BF16),
        pltpu.VMEM((2, chunks, 2, 2, 32, width), BF16),
        pltpu.VMEM((2, chunks, 2, 4, 32, width), BF16),
        pltpu.VMEM((2, chunks, 4, 32, width), BF16),
        pltpu.VMEM((2, chunks, 2, 16, width), BF16),
        pltpu.VMEM((2, chunks, 2, 32, width), BF16),
    ]


def gather_stages(rings, buf, ssem, rsem):
    def inner(h, k):
        ring = rings[1 - h]
        row = rings[h].me
        return (
            ring,
            lambda d: buf(h, k).at[row, d],
            lambda d, half: buf(h, k).at[row, d, pl.ds(16 * half, 16)],
        )

    def outer(h, k):
        return (
            rings[h],
            lambda d: buf(h, k).at[d],
            lambda d, half: buf(h, k).at[d, pl.ds(2 * half, 2)],
        )

    chunks = MLP_CHUNKS

    def start1(h, k, direct):
        ring, whole, block = inner(h, k)
        gather_start(ring, whole, block, ssem(h, k, 0), lambda i: rsem(h, k, i), direct)

    def forward1(k):
        @pl.when(k < chunks - STRAIGHT[2])
        def _():
            for h in range(2):
                ring, whole, block = inner(h, k)
                gather_forward(ring, whole, block, ssem(h, k, 0), lambda i: rsem(h, k, i))

    def start2(k):
        def finish(direct):
            for h in range(2):
                ring, whole, block = inner(h, k)
                gather_finish(ring, whole, block, lambda i: rsem(h, k, i), direct)

        def work(direct):
            for h in range(2):
                ring, whole, block = outer(h, k)
                gather_start(ring, whole, block, ssem(h, k, 1), lambda i: rsem(h, k, 4 + i), direct)

        either(k, chunks, STRAIGHT[2], finish)
        either(k, chunks, STRAIGHT[3], work)

    def forward2(k):
        @pl.when(k < chunks - STRAIGHT[3])
        def _():
            for h in range(2):
                ring, whole, block = outer(h, k)
                gather_forward(ring, whole, block, ssem(h, k, 1), lambda i: rsem(h, k, 4 + i))

    def finish2(k):
        def finish(direct):
            for h in range(2):
                ring, whole, block = outer(h, k)
                gather_finish(ring, whole, block, lambda i: rsem(h, k, 4 + i), direct)

        either(k, chunks, STRAIGHT[3], finish)

    def drain(h, k):
        wait_bytes(buf(h, k).at[0, pl.ds(0, 3)], ssem(h, k, 0))
        wait_bytes(buf(h, k).at[pl.ds(0, 3)], ssem(h, k, 1))

    return start1, forward1, start2, forward2, finish2, drain


def columns_sum(acc, full, mine, core_in, ring, y_in, ssem, rsem, meanwhile=None):
    core = lax.axis_index("c")

    def made(c, y):
        rows = []
        for i in range(2):
            z = 2 * c + i
            rows.append(acc[0, y, z] + acc[1, z, y])
        return jnp.concatenate(rows, axis=0)

    for r in (2, 1, 3, 0):
        place = ring.places[r]
        full[place] = made(1 - core, place).astype(BF16)
        send(full.at[place], core_in.at[place], ssem.at[0], rsem.at[r], {"c": 1 - core})
    for r in (2, 1, 3, 0):
        place = ring.places[r]
        both = made(core, place)
        wait_bytes(core_in.at[place], rsem.at[r])
        both = both + core_in[place].astype(F32)
        if r == 0:
            total = both
        else:
            mine[place] = both.astype(BF16)
            send(mine.at[place], y_in.at[r - 1], ssem.at[1], rsem.at[4], ring.devices[r])
    if meanwhile is not None:
        meanwhile()
    wait_bytes(y_in, rsem.at[4])
    total = total + jnp.sum(y_in[...].astype(F32), axis=0)
    wait_bytes(core_in, ssem.at[0])
    wait_bytes(y_in, ssem.at[1])
    return total


class PlaneGather:
    def __init__(self, rings, buf, ssem, rsem):
        self.rings, self.buf, self.ssem, self.rsem = rings, buf, ssem, rsem

    def block(self, h, r, piece):
        place = self.rings[1 - h].places[r]
        return self.buf.at[h, self.rings[h].me, place, pl.ds(16 * piece, 16)]

    def outward(self, h, r, piece):
        ref = self.block(h, r, piece)
        for way in (2, 1, 3):
            device = self.rings[h].devices[way]
            send(ref, ref, self.ssem.at[h, piece], self.rsem.at[h, piece, 2 + way], device)

    def start(self, piece):
        for h in range(2):
            ref = self.block(h, 0, piece)
            for way in (2, 1, 3):
                device = self.rings[1 - h].devices[way]
                send(ref, ref, self.ssem.at[h, piece], self.rsem.at[h, piece, way - 1], device)
        for h in range(2):
            self.outward(h, 0, piece)

    def relay(self, piece):
        for way in (1, 3, 2):
            for h in range(2):
                wait_bytes(self.block(h, 4 - way, piece), self.rsem.at[h, piece, way - 1])
                self.outward(h, 4 - way, piece)

    def finish(self, h, way, piece):
        place = self.rings[h].places[4 - way]
        wait_bytes(self.buf.at[h, place, :, pl.ds(16 * piece, 16)], self.rsem.at[h, piece, 2 + way])

    def drain(self):
        for h in range(2):
            for piece in range(2):
                wait_bytes(self.buf.at[h, 0, pl.ds(0, 3), pl.ds(0, 16)], self.ssem.at[h, piece])
                wait_bytes(self.buf.at[h, pl.ds(0, 3), :, pl.ds(0, 16)], self.ssem.at[h, piece])


def rotation(places):
    lane = lax.broadcasted_iota(jnp.int32, (1, HD), 1)
    index = lax.rem(lane, HD // 2).astype(F32)
    inv_freq = jnp.exp(index * (-2.0 * math.log(ROPE_BASE) / HD))
    angles = places * inv_freq
    sine = jnp.sin(angles)
    return jnp.cos(angles), jnp.where(lane < HD // 2, -sine, sine)


def layer_kernel(
    tok,
    h_attn_gain,
    h_mlp_gain,
    h_lengths,
    h_live_mask,
    w_qkv,
    keys,
    values,
    w_out,
    w_gate,
    w_up,
    w_down,
    base,
    extra,
    attn_gain,
    mlp_gain,
    lengths,
    live_mask,
    v_tok,
    v_qkv,
    v_keys,
    v_values,
    v_out,
    v_gate,
    v_up,
    v_down,
    qa_part,
    qa_in1,
    qa_sum1,
    qa_in2,
    qb_part,
    qb_in1,
    qb_sum1,
    qb_in2,
    sq0,
    sq0_x,
    sq0_mid,
    sq0_z,
    query,
    fresh,
    attended,
    lhs,
    abuf,
    acc,
    full,
    mine,
    core_in,
    y_in,
    full2,
    mine2,
    core_in2,
    y_in2,
    resid,
    part,
    far1,
    near1,
    sum1,
    far2,
    near2,
    hid,
    sq,
    sq_x,
    sq_mid,
    sq_z,
    scales,
    wsem,
    q_ssem,
    q_rsem,
    sqs0,
    a_ssem,
    a_rsem,
    y_ssem,
    y_rsem,
    r_ssem,
    r_rsem,
    sqs,
    m_ssem,
    m_rsem,
):
    rings = (Ring("x"), Ring("z"))
    yring = Ring("y")
    core = lax.axis_index("c")
    chunks, width = part.shape[1], part.shape[5]
    cut = width // 2
    depth = lhs.shape[4]
    slot0 = 32 * (4 * rings[0].me + rings[1].me)
    row0 = 64 * (2 * yring.me + core)
    loads = [
        pltpu.make_async_copy(src, dst, wsem.at[i])
        for i, (src, dst) in enumerate(
            (
                (tok, v_tok),
                (w_qkv, v_qkv),
                (keys, v_keys),
                (values, v_values),
                (w_out, v_out),
                (w_gate, v_gate),
                (w_up, v_up),
                (w_down, v_down),
            )
        )
    ]
    small = [
        pltpu.make_async_copy(src, dst, wsem.at[8 + i])
        for i, (src, dst) in enumerate(
            (
                (h_attn_gain, attn_gain),
                (h_mlp_gain, mlp_gain),
                (h_lengths, lengths),
                (h_live_mask, live_mask),
            )
        )
    ]
    loads[0].start()
    for load in small:
        load.start()
    loads[1].start()
    met = greet(
        [*rings[0].devices[1:], *rings[1].devices[1:], *yring.devices[1:], {"c": 1 - core}]
    )

    def row(ref):
        return ref[...].astype(F32).reshape(1, ref.shape[0])

    def normed(a, wide, gain):
        scaled = (wide * gain).astype(BF16).reshape(4, 32, depth)
        lhs[0, a] = scaled
        for b in range(4):
            lhs[1, b, a] = scaled[b]

    for load in small:
        load.wait()
    loads[0].wait()
    for a in range(4):
        normed(a, v_tok[128 * a : 128 * (a + 1), :].astype(F32), row(attn_gain))
    loads[1].wait()
    for load in loads[2:]:
        load.start()
    squares0 = Squares(rings, sq0, sq0_x, sq0_mid, sq0_z, sqs0)
    squares = Squares(rings, sq, sq_x, sq_mid, sq_z, sqs)
    pieces = (
        (qa_part, qa_in1, qa_sum1, qa_in2, 0, 3),
        (qb_part, qb_in1, qb_sum1, qb_in2, 3, 5),
    )
    for p, (q_part, q_in1, _, _, begin, end) in enumerate(pieces):
        width_q = HD * (end - begin)
        for h in range(2):
            columns = slice(HD * (5 * h + begin), HD * (5 * h + end))
            got = jnp.dot(lhs[h].reshape(512, depth), v_qkv[:, columns], preferred_element_type=F32)
            q_part[h] = got.astype(BF16).reshape(4, 4, 32, width_q)
            if p == 0 and h == 0:
                met()
            scatter_direct(
                rings[h],
                lambda d: q_part.at[h, d],
                lambda i: q_in1.at[h, i],
                q_ssem.at[p, h, 0],
                q_rsem.at[p, h, 0],
            )
    for a in range(4):
        sq0[a] = row_squares(v_tok[128 * a : 128 * (a + 1), :].astype(F32))
    squares0.over_x()
    places = as_column(row(lengths), 32, slot0)
    cosine, sine = rotation(places)
    fresh[:, 2, :] = jnp.broadcast_to(places, (32, 128))
    for p, (q_part, q_in1, q_sum1, q_in2, _, _) in enumerate(pieces):
        for h in range(2):
            wait_bytes(q_in1.at[h], q_rsem.at[p, h, 0])
            total = q_part[h, rings[h].me].astype(F32)
            for i in range(3):
                total = total + q_in1[h, i].astype(F32)
            q_sum1[h] = total.astype(BF16)
            scatter_direct(
                rings[1 - h],
                lambda d: q_sum1.at[h, d],
                lambda i: q_in2.at[h, i],
                q_ssem.at[p, h, 1],
                q_rsem.at[p, h, 1],
            )
        if p == 0:
            squares0.over_z()
    scale = squares0.scale()
    for p, (_, _, q_sum1, q_in2, begin, end) in enumerate(pieces):
        for h in range(2):
            wait_bytes(q_in2.at[h], q_rsem.at[p, h, 1])
            total = q_sum1[h, rings[1 - h].me].astype(F32)
            for i in range(3):
                total = total + q_in2[h, i].astype(F32)
            sums = total * scale
            for i in range(end - begin):
                column = sums[:, 128 * i : 128 * (i + 1)]
                head = 5 * h + begin + i
                if head < 9:
                    column = column * cosine + pltpu.roll(column, HD // 2, 1) * sine
                column = column.astype(BF16).astype(F32)
                if head < 8:
                    query[:, head, :] = column
                else:
                    fresh[:, head - 8, :] = column

    loads[2].wait()
    loads[3].wait()

    def slots(g, carry):
        first = 8 * g
        score_scale = HD ** (-0.5)
        q = query[pl.ds(first, 8)]
        scores = []
        for i in range(8):
            scores.append(
                lax.dot_general(
                    q[i].astype(BF16),
                    v_keys[first + i],
                    (((1,), (1,)), ((), ())),
                    preferred_element_type=F32,
                )
            )
        scores = jnp.concatenate(scores, axis=0) * score_scale
        new = fresh[pl.ds(first, 8)]
        q = q.reshape(64, HD)

        def spread(i):
            return jnp.broadcast_to(new[:, i : i + 1, :], (8, 8, HD)).reshape(64, HD)

        own = jnp.sum(q * spread(0), axis=1, keepdims=True) * score_scale
        ends = spread(2)[:, 0:1]
        spot = lax.broadcasted_iota(jnp.int32, scores.shape, 1).astype(F32)
        valid = spot < ends
        scores = jnp.where(valid, scores, MASKED)
        peak = jnp.maximum(jnp.max(scores, axis=1, keepdims=True), own)
        probs = jnp.where(valid, jnp.exp(scores - peak), 0.0).astype(BF16).astype(F32)
        own_weight = jnp.exp(own - peak).astype(BF16).astype(F32)
        totals = jnp.sum(probs, axis=1, keepdims=True) + own_weight
        blends = []
        for i in range(8):
            blends.append(
                jnp.dot(
                    probs[8 * i : 8 * (i + 1)].astype(BF16),
                    v_values[first + i],
                    preferred_element_type=F32,
                )
            )
        blend = jnp.concatenate(blends, axis=0) + own_weight * spread(1)
        attended[pl.ds(first, 8)] = (blend / totals).reshape(8, 8, HD)
        return carry

    gather = PlaneGather(rings, abuf, a_ssem, a_rsem)
    for piece in range(2):
        lax.fori_loop(2 * piece, 2 * piece + 2, slots, 0)
        rows = pl.ds(16 * piece, 16)
        for head in range(8):
            h, i = divmod(head, 4)
            abuf[h, rings[h].me, rings[1 - h].me, rows, 128 * i : 128 * (i + 1)] = attended[
                rows, head, :
            ].astype(BF16)
        gather.start(piece)
    for piece in range(2):
        gather.relay(piece)
    half = abuf.shape[4]
    loads[4].wait()
    for h in range(2):
        for piece in range(2):
            for way in (1, 3, 2):
                gather.finish(h, way, piece)
        block = abuf[h].reshape(512, half)
        got = jnp.dot(block, v_out[h * half : (h + 1) * half, :], preferred_element_type=F32)
        acc[h] = got.reshape(4, 4, 32, acc.shape[4])
    total = columns_sum(acc, full, mine, core_in, yring, y_in, y_ssem.at[0], y_rsem.at[0])
    live = as_column(row(live_mask), 64, row0)
    kept = (v_tok[pl.ds(pl.multiple_of(row0, 64), 64), :].astype(F32) + live * total).astype(BF16)

    def r_whole(d):
        return resid.at[d, core]

    def to_core(r):
        ref = r_whole(yring.places[r])
        send(ref, ref, r_ssem.at[1], r_rsem.at[3 + r], {"c": 1 - core})

    def take(r):
        place = yring.places[r]
        wait_bytes(resid.at[place, 1 - core], r_rsem.at[3 + r])
        normed(place, resid[place].astype(F32).reshape(128, depth), row(mlp_gain))

    resid[yring.me, core] = kept
    gather_direct(yring, r_whole, r_ssem.at[0], lambda i: r_rsem.at[i])
    to_core(0)
    acc[...] = jnp.zeros_like(acc)
    take(0)
    for r in (1, 3, 2):
        wait_bytes(r_whole(yring.places[4 - r]), r_rsem.at[r - 1])
        to_core(4 - r)
    for r in (1, 3, 2):
        take(4 - r)
    for load in loads[5:]:
        load.wait()

    s_start1, s_forward1, s_start2, s_forward2, s_finish2 = scatter_stages(
        rings, part, far1, near1, sum1, far2, near2, m_ssem, m_rsem
    )
    g_start1, g_forward1, g_start2, g_forward2, g_finish2, g_drain = gather_stages(
        rings,
        lambda h, k: hid.at[h, k],
        lambda h, k, i: m_ssem.at[k, h, 2 + i],
        lambda h, k, i: m_rsem.at[k, h, 8 + i],
    )

    def compute(k):
        for h in range(2):
            cols = pl.ds(pl.multiple_of((2 * k + h) * cut, 128), cut)
            block = lhs[h].reshape(512, depth)
            for i, v in enumerate((v_gate, v_up)):
                got = jnp.dot(block, v[:, cols], preferred_element_type=F32)
                part[h, k, :, :, :, i * cut : (i + 1) * cut] = got.astype(BF16).reshape(
                    4, 4, 32, cut
                )
            s_start1(h, k)

        @pl.when(k == 1)
        def _():
            for a in range(4):
                sq[a] = row_squares(resid[a].astype(F32).reshape(128, depth))
            squares.over_x()

    def hidden(k):
        @pl.when(k == 0)
        def _():
            scales[...] = jnp.broadcast_to(squares.scale(), scales.shape)

        scale = scales[:, 0:1]

        def work(direct):
            for h in range(2):
                sums = s_finish2(h, k, direct) * scale
                gate = sums[:, :cut]
                up = sums[:, cut:]
                made = gate * (1.0 / (1.0 + jnp.exp(-gate))) * up
                hid[h, k, rings[h].me, rings[1 - h].me] = made.astype(BF16)

        def go(direct):
            for h in range(2):
                g_start1(h, k, direct)

        either(k, chunks, STRAIGHT[1], work)
        either(k, chunks, STRAIGHT[2], go)

    def down(k):
        g_finish2(k)
        for h in range(2):
            depths = pl.ds(pl.multiple_of((2 * k + h) * cut, 128), cut)
            block = hid[h, k].reshape(512, cut)
            got = jnp.dot(block, v_down[depths, :], preferred_element_type=F32)
            acc[h] += got.reshape(4, 4, 32, acc.shape[4])

    def forward1(k):
        @pl.when(k == 1)
        def _():
            squares.over_z()

        s_forward1(k)

    run_stages(
        chunks,
        (compute, forward1, s_start2, s_forward2, hidden, g_forward1, g_start2, g_forward2, down),
    )

    def settle():
        squares0.drain()
        squares.drain()
        gather.drain()
        for p, (_, q_in1, _, q_in2, _, _) in enumerate(pieces):
            for h in range(2):
                wait_bytes(q_in1.at[h], q_ssem.at[p, h, 0])
                wait_bytes(q_in2.at[h], q_ssem.at[p, h, 1])
        wait_bytes(resid.at[pl.ds(0, 3), 0], r_ssem.at[0])
        wait_bytes(resid.at[:, 0], r_ssem.at[1])

        def drain(k, carry):
            for h in range(2):
                wait_bytes(part.at[h, k, pl.ds(0, 3)], m_ssem.at[k, h, 0])
                wait_bytes(sum1.at[h, k, pl.ds(0, 3)], m_ssem.at[k, h, 1])
                g_drain(h, k)
            return carry

        lax.fori_loop(0, chunks, drain, 0)

    sems = (y_ssem.at[1], y_rsem.at[1])
    total = columns_sum(acc, full2, mine2, core_in2, yring, y_in2, *sems, settle)
    base[...] = kept
    extra[...] = live * total


def q_scratch(width):
    return [
        pltpu.VMEM((2, 4, 4, 32, width), BF16),
        pltpu.VMEM((2, 3, 4, 32, width), BF16),
        pltpu.VMEM((2, 4, 32, width), BF16),
        pltpu.VMEM((2, 3, 32, width), BF16),
    ]


def layer_rows(tok, attn_gain, mlp_gain, lengths, live_mask, w_qkv, keys, values, w_out, w_gate, w_up, w_down):
    depth = w_gate.shape[0]
    cut = w_gate.shape[1] // (2 * MLP_CHUNKS)
    half = w_out.shape[0] // 2
    across = w_out.shape[1]
    slots = keys.shape[0]
    vmem = pl.BlockSpec(memory_space=pltpu.VMEM)
    hbm = pl.BlockSpec(memory_space=pl.ANY)
    held = (tok, w_qkv, keys, values, w_out, w_gate, w_up, w_down)
    squares = [
        pltpu.VMEM((4, 8, 128), F32),
        pltpu.VMEM((3, 8, 128), F32),
        pltpu.VMEM((8, 128), F32),
        pltpu.VMEM((3, 8, 128), F32),
    ]
    sums = [
        pltpu.VMEM((4, 64, across), BF16),
        pltpu.VMEM((4, 64, across), BF16),
        pltpu.VMEM((4, 64, across), BF16),
        pltpu.VMEM((3, 64, across), BF16),
    ]
    return pl.pallas_call(
        layer_kernel,
        name="layer_rows",
        out_shape=(
            jax.ShapeDtypeStruct((64, across), BF16),
            jax.ShapeDtypeStruct((64, across), F32),
        ),
        in_specs=[hbm] * 12,
        out_specs=(vmem, vmem),
        scratch_shapes=[
            *[pltpu.VMEM(a.shape, a.dtype) for a in (attn_gain, mlp_gain, lengths, live_mask)],
            *[pltpu.VMEM(a.shape, BF16) for a in held],
            *q_scratch(3 * HD),
            *q_scratch(2 * HD),
            *squares,
            pltpu.VMEM((slots, 8, HD), F32),
            pltpu.VMEM((slots, 8, HD), F32),
            pltpu.VMEM((slots, 8, HD), F32),
            pltpu.VMEM((2, 4, 4, 32, depth), BF16),
            pltpu.VMEM((2, 4, 4, 32, half), BF16),
            pltpu.VMEM((2, 4, 4, 32, across), F32),
            *sums,
            *sums,
            pltpu.VMEM((4, 2, 64, across), BF16),
            *scatter_scratch(MLP_CHUNKS, 2 * cut),
            pltpu.VMEM((2, MLP_CHUNKS, 4, 4, 32, cut), BF16),
            *squares,
            pltpu.VMEM((32, 128), F32),
            pltpu.SemaphoreType.DMA((12,)),
            pltpu.SemaphoreType.DMA((2, 2, 2)),
            pltpu.SemaphoreType.DMA((2, 2, 2)),
            pltpu.SemaphoreType.DMA((4,)),
            pltpu.SemaphoreType.DMA((2, 2)),
            pltpu.SemaphoreType.DMA((2, 2, 6)),
            pltpu.SemaphoreType.DMA((2, 2)),
            pltpu.SemaphoreType.DMA((2, 5)),
            pltpu.SemaphoreType.DMA((2,)),
            pltpu.SemaphoreType.DMA((7,)),
            pltpu.SemaphoreType.DMA((4,)),
            pltpu.SemaphoreType.DMA((MLP_CHUNKS, 2, 4)),
            pltpu.SemaphoreType.DMA((MLP_CHUNKS, 2, 16)),
        ],
        compiler_params=pltpu.CompilerParams(
            collective_id=0, has_side_effects=True, vmem_limit_bytes=60 * 1024 * 1024
        ),
    )(tok, attn_gain, mlp_gain, lengths, live_mask, w_qkv, keys, values, w_out, w_gate, w_up, w_down)


def per_device(
    tokens,
    attn_gain,
    qkv_weight,
    cache_keys,
    cache_values,
    lengths,
    live_mask,
    out_weight,
    mlp_gain,
    gate_weight,
    up_weight,
    down_weight,
):
    base, extra = layer_rows(
        tokens,
        attn_gain,
        mlp_gain,
        lengths,
        live_mask,
        qkv_weight,
        cache_keys.reshape(cache_keys.shape[0], *cache_keys.shape[2:]),
        cache_values.reshape(cache_values.shape[0], *cache_values.shape[2:]),
        out_weight,
        gate_weight,
        up_weight,
        down_weight,
    )
    return (base.astype(F32) + extra).astype(BF16)


def solution(mesh):
    finer = Mesh(mesh.devices.reshape(4, 4, 4, 2), ("x", "z", "y", "c"))
    return jax.shard_map(
        per_device,
        mesh=finer,
        in_specs=(
            P(None, GX),
            P(GX),
            P(GX, GY),
            P(GX, GY, None, None),
            P(GX, GY, None, None),
            P(),
            P(),
            P(GY, GX),
            P(GX),
            P(GX, GY),
            P(GX, GY),
            P(GY, GX),
        ),
        out_specs=P(GY, GX),
        check_vma=False,
    )
```
